128 devices in a mesh: px: 16 (over x, z_hi, core), py: 8 (over z_lo, y).
Axes of the slice: x: 4, y: 4, z: 4 (z_hi: 2, z_lo: 2; z = z_hi * 2 + z_lo), core: 2. Of those that a mesh axis runs over, the one named last changes fastest.
Arguments:
- state: float32 [4, 128, 16, 4096], P(None, ('px', 'py')), may hold values from -6 to 6
- past_slow: float32 [4, 128, 16, 4096], P(None, ('px', 'py')), may hold values from -6 to 6
- mean_wind: float32 [128], P(('px', 'py')), may hold values from -2 to 2
- damping: float32 [128], P(('px', 'py')), may hold values from 0.05 to 1
- vertical_inverse: float32 [256, 256], replicated, as said below
- section: int32 [8], replicated, may hold values from 0 to 3
Outputs:
- advanced: float32 [4, 128, 16, 4096], P(None, ('px', 'py'))
The draws below stay inside these ranges and needn't reach their ends.
Inputs may be any that keep to these rules, and one draw needn't show every extreme that they name: `section`: row of the four-row coupling coefficient table for each substep. `vertical_inverse`: the inverse of a nonsingular vertical acoustic operator for 128 levels of vertical velocity followed by 128 levels of pressure.
All inputs are finite; a program needn't handle non-finite values.
Results may differ from the reference program's by a relative error of at most 0.00015.
Values sent between devices are 32-bit elements; how exact they have to be, the bound alone decides.
No kernel may reach another device: no remote copies, remote signals or barrier semaphores. Data moves between devices by JAX's collectives and lax.ppermute only.
A program may use at most 128 MiB of HBM per device.

```python
import math
import jax
import jax.numpy as jnp
from jax import lax

NX = 4096
NZ = 128
SUBSTEPS = 8
NY = 16


def draw_vertical_inverse(key, part):
    order = 2 * NZ
    first_key = jax.random.fold_in(key, 11)
    second_key = jax.random.fold_in(key, 12)
    diagonal = jax.random.uniform(first_key, (order,), jnp.float32, 0.6, 1.4)
    spread = jax.random.normal(second_key, (order, order), jnp.float32) * (0.35 / math.sqrt(order))
    return spread + jnp.diag(diagonal)


def touch_ends(drawn, stream_key, low, top_value):
    longest = drawn.shape.index(max(drawn.shape))
    spots = []
    for shift in (0, 1):
        where = [jax.random.randint(jax.random.fold_in(stream_key, axis), (), 0, length) for axis, length in enumerate(drawn.shape)]
        where[longest] = (where[longest] + shift) % drawn.shape[longest]
        spots.append(tuple(where))
    return drawn.at[spots[0]].set(low).at[spots[1]].set(top_value)


def levels(stream_key, extent, shards, smallest, high):
    def one(dim, parts):
        draws = jax.random.uniform(jax.random.fold_in(jax.random.fold_in(stream_key, 6), dim), (parts,), jnp.float32, smallest / len(shards), high / len(shards))
        return jnp.repeat(jnp.exp(draws), extent[dim] // parts).reshape((-1,) + (1,) * (len(extent) - dim - 1))

    loudness = one(*shards[0])
    for cut in shards[1:]:
        loudness = loudness * one(*cut)
    return loudness


def scatter_about(key, extent, width, most, split=(), kind=jnp.bfloat16):
    gain = levels(key, extent, split, -0.22, 0.18) if split else 1.0
    drawn = jax.random.normal(key, extent, jnp.float32) * width * gain
    return jnp.minimum(jnp.maximum(drawn, -most), most).astype(kind)


def setup_inputs(seed: int = 0) -> dict:
    keys = jax.random.split(jax.random.key(seed), 7)
    state = scatter_about(keys[0], (4, NZ, NY, NX), 1.0, 6.0, ((1, 128),), jnp.float32)
    past_slow = scatter_about(keys[1], (4, NZ, NY, NX), 1.0, 6.0, ((1, 128),), jnp.float32)
    mean_wind = jnp.clip(jax.random.uniform(keys[2], (NZ,), jnp.float32, -2.0, 2.0) * levels(keys[2], (NZ,), ((0, 128),), -0.4, 0.0), -2.0, 2.0)
    damping = jnp.clip(jnp.exp(math.log(1.0) - 2.9957323 * jax.random.uniform(keys[3], (NZ,), jnp.float32) ** levels(keys[3], (NZ,), ((0, 128),), -0.2, 0.2)), 0.05, 1.0)
    vertical_inverse = draw_vertical_inverse(jax.random.fold_in(keys[6], 71), 0)
    section = touch_ends(jax.random.randint(keys[5], (SUBSTEPS,), 0, 4), jax.random.fold_in(keys[5], 1), 0, 3).astype(jnp.int32)
    return {"state": state, "past_slow": past_slow, "mean_wind": mean_wind, "damping": damping, "vertical_inverse": vertical_inverse, "section": section}


now_weights = (-1.0, 2.0, 0.5, 1.5)
past_weights = (1.0, -0.5, 0.25, -1.0)
courant = 0.55


def section_weights(section):
    rows_all = jnp.arange(4, dtype=jnp.int32)
    picked = (section[:, None] == rows_all[None, :]).astype(jnp.float32)
    weight_now = jnp.sum(picked * jnp.array(now_weights, jnp.float32)[None, :], axis=1)
    weight_past = jnp.sum(picked * jnp.array(past_weights, jnp.float32)[None, :], axis=1)
    return weight_now, weight_past


def slow_field(field_one, mean_wind, damping):
    modes = jnp.arange(NX // 2 + 1, dtype=jnp.int32)
    wavenum = modes.astype(jnp.float32) * (2.0 * math.pi / NX)
    slope = jnp.where(modes == NX // 2, 0.0, wavenum)
    real_part = -damping[:, None] * (wavenum[None, :] / math.pi) ** 4
    imag_part = -mean_wind[:, None] * slope[None, :]
    spectrum = jnp.fft.rfft(field_one, axis=-1)
    scaled = spectrum * (real_part + 1j * imag_part)[:, None, :]
    return jnp.fft.irfft(scaled, n=NX, axis=-1).astype(jnp.float32)


def vertical_diff(field_one):
    padded = jnp.pad(field_one, ((1, 1), (0, 0), (0, 0)))
    return padded[2:] - padded[:-2]


def reference(state, past_slow, mean_wind, damping, vertical_inverse, section):
    weight_now, weight_past = section_weights(section)
    slow = lax.map(lambda field_one: slow_field(field_one, mean_wind, damping), state)
    upright = state[2:4].reshape(2 * NZ, NY * NX)
    solved = jnp.dot(vertical_inverse, upright, precision=lax.Precision.HIGHEST,
                     preferred_element_type=jnp.float32).reshape(2, NZ, NY, NX)
    along_x = state[0]
    along_y = state[1]
    upward = solved[0]
    pressure = solved[1]
    half_step = 0.5 * courant
    fast_step = 1.0 / SUBSTEPS
    for substep in range(SUBSTEPS):
        forcing = weight_now[substep] * slow + weight_past[substep] * past_slow
        along_x = along_x - half_step * (jnp.roll(pressure, -1, 2) - jnp.roll(pressure, 1, 2)) + fast_step * forcing[0]
        along_y = along_y - half_step * (jnp.roll(pressure, -1, 1) - jnp.roll(pressure, 1, 1)) + fast_step * forcing[1]
        upward = upward - half_step * vertical_diff(pressure) + fast_step * forcing[2]
        spread = (jnp.roll(along_x, -1, 2) - jnp.roll(along_x, 1, 2)) + (jnp.roll(along_y, -1, 1) - jnp.roll(along_y, 1, 1)) + vertical_diff(upward)
        pressure = pressure - half_step * spread + fast_step * forcing[3]
    return jnp.stack([along_x, along_y, upward, pressure])
```

```python
import math

import jax
import jax.numpy as jnp
import numpy as np
from jax import lax
from jax.experimental import pallas as pl
from jax.experimental.pallas import tpu as pltpu
from jax.sharding import PartitionSpec as P

SUBSTEPS = 8
NX, NY, NZ = 4096, 16, 128
N1, N2 = 32, 128
KAP = NY // 2
HALF = 0.275
FAST = 1.0 / SUBSTEPS
NOW = (-1.0, 2.0, 0.5, 1.5)
PAST = (1.0, -0.5, 0.25, -1.0)
ROWS_IN = 25
ROWS_OUT = 12

f32 = jnp.float32
bf16 = jnp.bfloat16


def halves(table):
    high = jnp.asarray(table, f32).astype(bf16)
    low = jnp.asarray(np.asarray(table, np.float64) - np.asarray(high, np.float64), bf16)
    return np.stack([np.asarray(high), np.asarray(low)])


def tables():
    n1 = np.arange(N1)
    y = np.arange(NY)
    kap = np.arange(KAP)
    qa = np.cos(2 * np.pi * kap[:, None] * y[None, :] / NY) * math.sqrt(2.0 / NY)
    qb = np.sin(2 * np.pi * kap[:, None] * y[None, :] / NY) * math.sqrt(2.0 / NY)
    qa[0] = 1.0 / math.sqrt(NY)
    qb[0] = (-1.0) ** y / math.sqrt(NY)
    q = qa + 1j * qb
    dft1 = np.exp(-2j * np.pi * (n1[:, None] * n1[None, :] % N1) / N1)
    stage = np.einsum("kn,cy->kcny", dft1, q).reshape(N1, KAP, N1, 2, 8)
    stage = stage.transpose(0, 1, 3, 2, 4).reshape(N1 * KAP, 2 * N1 * 8)
    first = np.concatenate([stage.real, stage.imag], 0)
    last = first.T / NX
    n2 = np.arange(N2)
    angle = 2 * np.pi * (n2[:, None] * n2[None, :] % N2) / N2
    cos, sin = np.cos(angle), np.sin(angle)
    second = np.block([[cos, sin], [-sin, cos]])
    turn = 2 * np.pi * (n1[:, None] * n2[None, :]) / NX
    twist = np.stack([np.cos(turn), np.sin(turn)]).astype(np.float32)
    wide = np.repeat(turn.T, KAP, axis=1)
    untwist = np.stack([np.cos(wide), np.sin(wide)]).astype(np.float32)
    return halves(first), halves(last), halves(second), halves(second.T), twist, untwist


FIRST, LAST, SECOND, SECOND_BACK, TWIST, UNTWIST = tables()


def split(value):
    high = value.astype(bf16)
    return high, (value - high.astype(f32)).astype(bf16)


def product(left, right, dims=((1,), (0,))):
    def dot(a, b):
        return lax.dot_general(a, b, (dims, ((), ())), preferred_element_type=f32)

    return dot(left[0], right[0]) + (dot(left[1], right[0]) + dot(left[0], right[1]))


ACROSS = ((1,), (1,))


def tiles(plane):
    return jnp.concatenate(
        [plane[8 * b : 8 * b + 8, N2 * n : N2 * n + N2] for b in range(2) for n in range(N1)], axis=0
    )


def forward(columns, first, second, twist):
    mid = product(first, split(columns))
    real, imag = [], []
    for k in range(N1):
        zr = mid[8 * k : 8 * k + 8]
        zi = mid[256 + 8 * k : 256 + 8 * k + 8]
        c, s = twist[0, k : k + 1, :], twist[1, k : k + 1, :]
        real.append(zr * c + zi * s)
        imag.append(zi * c - zr * s)
    turned = jnp.concatenate([jnp.concatenate(real, 0), jnp.concatenate(imag, 0)], axis=1)
    return product(second, split(turned), ACROSS)


def backward(modes, last, second_back, untwist):
    mid = product(second_back, split(modes))
    zr, zi = mid[:N2], mid[N2:]
    c, s = untwist[0], untwist[1]
    turned = jnp.concatenate([zr * c - zi * s, zr * s + zi * c], axis=1)
    return product(last, split(turned), ACROSS)


def pair(ref):
    return ref[0], ref[1]


def diff_x(plane):
    return pltpu.roll(plane, NX - 1, 1) - pltpu.roll(plane, 1, 1)


def diff_y(plane):
    return pltpu.roll(plane, NY - 1, 0) - pltpu.roll(plane, 1, 0)


def send_kernel(wind, damping, state, past, first, second, twist, out):
    first, second = pair(first), pair(second)
    for which, source in enumerate((state, past)):
        for index in range(3):
            if index == 0:
                plane = diff_x(source[0, 0]) + diff_y(source[1, 0])
            else:
                plane = source[index + 1, 0]
            modes = forward(tiles(plane), first, second, twist)
            for part in range(4):
                block = modes[N2 * (part // 2) : N2 * (part // 2) + N2, 128 * (part % 2) : 128 * (part % 2) + 128]
                out[pl.ds(12 * which + 4 * index + part, N2, stride=ROWS_IN), :] = block
    lane = lax.broadcasted_iota(jnp.int32, (N2, 128), 1)
    out[pl.ds(24, N2, stride=ROWS_IN), :] = jnp.where(lane < 64, damping[0], wind[0])


def weight(section, table, step):
    row = section[step]
    value = jnp.where(row == 3, table[3], 0.0)
    for entry in range(3):
        value = jnp.where(row == entry, table[entry], value)
    return value


def local_kernel(wind, damping, section, state, past, first, last, second, second_back, twist, untwist, out):
    total_now = weight(section, NOW, 0)
    total_past = weight(section, PAST, 0)
    for step in range(1, SUBSTEPS):
        total_now = total_now + weight(section, NOW, step)
        total_past = total_past + weight(section, PAST, step)
    k = lax.broadcasted_iota(jnp.int32, (N2, 256), 0) * N1 + lax.broadcasted_iota(jnp.int32, (N2, 256), 1) // KAP
    fold = jnp.minimum(k, NX - k).astype(f32) * (2.0 / NX)
    fold = fold * fold
    signed = jnp.where(k > NX // 2, k - NX, k)
    signed = jnp.where(k == NX // 2, 0, signed).astype(f32) * (2.0 * math.pi / NX)
    damp = (fold * fold) * (damping[0] * -1.0)
    drift = signed * wind[0]
    for index in range(2):
        modes = forward(tiles(state[index, 0]), pair(first), pair(second), twist)
        fr, fi = modes[:N2], modes[N2:]
        scaled = jnp.concatenate([damp * fr + drift * fi, damp * fi - drift * fr], axis=0)
        slow = backward(scaled, pair(last), pair(second_back), untwist)
        for b in range(2):
            for n in range(N1):
                rows, cols = slice(8 * b, 8 * b + 8), slice(N2 * n, N2 * n + N2)
                piece = slow[8 * (b * N1 + n) : 8 * (b * N1 + n) + 8]
                out[index, rows, cols] = state[index, 0, rows, cols] + FAST * (
                    total_now * piece + total_past * past[index, 0, rows, cols]
                )


def column_kernel(section, lanes, inverse, got, out, chi, slow, up, press, total):
    zero = jnp.zeros((8, 128), f32)
    params = got[pl.ds(24, NZ, stride=ROWS_IN), :]
    damping, wind = params[:, 0:1], params[:, 64:65]

    def plane(which, index, part):
        return got[pl.ds(12 * which + 4 * index + part, NZ, stride=ROWS_IN), :]

    for tile in range(2):
        at = slice(128 * tile, 128 * tile + 128)
        damp = -damping * lanes[0:1, at]
        drift = wind * lanes[1:2, at]
        for index in range(3):
            fr, fi = plane(0, index, tile), plane(0, index, 2 + tile)
            slow[index, tile] = damp * fr + drift * fi
            slow[index, 2 + tile] = damp * fi - drift * fr
            if index == 0:
                chi[tile] = fr
                chi[2 + tile] = fi
    inv = split(inverse[...])
    for part in range(4):
        upright = jnp.concatenate([plane(0, 1, part), plane(0, 2, part)], axis=0)
        solved = product(inv, split(upright))
        up[part, 8 : 8 + NZ] = solved[:NZ]
        press[part, 8 : 8 + NZ] = solved[NZ:]
        total[part] = jnp.zeros((NZ, 128), f32)
        for ref in (up, press):
            ref[part, 0:8] = zero
            ref[part, 8 + NZ : 16 + NZ] = zero

    def step_body(step, carry):
        now = weight(section, NOW, step) * FAST
        then = weight(section, PAST, step) * FAST
        for part in range(4):
            at = slice(128 * (part % 2), 128 * (part % 2) + 128)
            coupling = lanes[2:3, at]
            p = press[part, 8 : 8 + NZ]
            fresh = chi[part] + coupling * p + (now * slow[0, part] + then * plane(1, 0, part))
            chi[part] = fresh
            total[part] = total[part] + p
            up[part, 8 : 8 + NZ] = (
                up[part, 8 : 8 + NZ]
                - HALF * (press[part, 9 : 9 + NZ] - press[part, 7 : 7 + NZ])
                + (now * slow[1, part] + then * plane(1, 1, part))
            )
            press[part, 8 : 8 + NZ] = (
                p
                - HALF * (fresh + (up[part, 9 : 9 + NZ] - up[part, 7 : 7 + NZ]))
                + (now * slow[2, part] + then * plane(1, 2, part))
            )
        return carry

    lax.fori_loop(0, SUBSTEPS, step_body, 0)
    for part in range(4):
        out[pl.ds(part, NZ, stride=ROWS_OUT), :] = total[part]
        out[pl.ds(4 + part, NZ, stride=ROWS_OUT), :] = up[part, 8 : 8 + NZ]
        out[pl.ds(8 + part, NZ, stride=ROWS_OUT), :] = press[part, 8 : 8 + NZ]


def finish_kernel(got, side, last, second_back, untwist, out):
    for index in range(3):
        parts = [got[pl.ds(4 * index + part, N2, stride=ROWS_OUT), :] for part in range(4)]
        modes = jnp.concatenate(
            [jnp.concatenate(parts[:2], axis=1), jnp.concatenate(parts[2:], axis=1)], axis=0
        )
        real = backward(modes, pair(last), pair(second_back), untwist)
        if index:
            for b in range(2):
                for n in range(N1):
                    out[index + 1, 0, 8 * b : 8 * b + 8, N2 * n : N2 * n + N2] = real[
                        8 * (b * N1 + n) : 8 * (b * N1 + n) + 8
                    ]
        else:
            plane = jnp.concatenate(
                [
                    jnp.concatenate([real[8 * (b * N1 + n) : 8 * (b * N1 + n) + 8] for n in range(N1)], axis=1)
                    for b in range(2)
                ],
                axis=0,
            )
            out[0, 0] = side[0] - HALF * diff_x(plane)
            out[1, 0] = side[1] - HALF * diff_y(plane)


def lane_tables(index):
    k = index * N1 + jnp.arange(256, dtype=jnp.int32) // KAP
    wavenum = jnp.minimum(k, NX - k).astype(f32) * (2.0 / NX)
    wavenum = wavenum * wavenum
    signed = jnp.where(k > NX // 2, k - NX, k)
    signed = jnp.where(k == NX // 2, 0, signed).astype(f32) * (2.0 * math.pi / NX)
    sx = jnp.sin(k.astype(f32) * (2.0 * math.pi / NX))
    sy = jnp.sin((jnp.arange(256) % KAP).astype(f32) * (2.0 * math.pi / NY))
    coupling = (4.0 * HALF) * (sx * sx + sy * sy)
    rows = [wavenum * wavenum, signed, coupling]
    return jnp.stack(rows + [jnp.zeros_like(coupling)] * 5)


VMEM = pl.BlockSpec(memory_space=pltpu.VMEM)
SMEM = pl.BlockSpec(memory_space=pltpu.SMEM)


def local(state, past_slow, mean_wind, damping, vertical_inverse, section):
    axes = ("px", "py")
    message = pl.pallas_call(
        send_kernel,
        out_shape=jax.ShapeDtypeStruct((NZ * ROWS_IN, 128), f32),
        in_specs=[SMEM, SMEM] + [VMEM] * 5,
        out_specs=VMEM,
        name="send",
    )(mean_wind, damping, state, past_slow, FIRST, SECOND, TWIST)
    got = lax.all_to_all(message.reshape(NZ, ROWS_IN, 1, 128), axes, split_axis=0, concat_axis=0, tiled=True)
    side = pl.pallas_call(
        local_kernel,
        out_shape=jax.ShapeDtypeStruct((2, NY, NX), f32),
        in_specs=[SMEM, SMEM, SMEM] + [VMEM] * 8,
        out_specs=VMEM,
        cost_estimate=pl.CostEstimate(flops=8_000_000_000, bytes_accessed=4_000_000, transcendentals=0),
        name="side",
    )(mean_wind, damping, section, state, past_slow, FIRST, LAST, SECOND, SECOND_BACK, TWIST, UNTWIST)
    lanes = lane_tables(lax.axis_index(axes))
    padded = pltpu.VMEM((4, NZ + 16, 128), f32)
    solved = pl.pallas_call(
        column_kernel,
        out_shape=jax.ShapeDtypeStruct((NZ * ROWS_OUT, 128), f32),
        in_specs=[SMEM] + [VMEM] * 3,
        out_specs=VMEM,
        scratch_shapes=[
            pltpu.VMEM((4, NZ, 128), f32),
            pltpu.VMEM((3, 4, NZ, 128), f32),
            padded,
            padded,
            pltpu.VMEM((4, NZ, 128), f32),
        ],
        name="columns",
    )(section, lanes, vertical_inverse, got.reshape(NZ * ROWS_IN, 128))
    back = lax.all_to_all(
        solved.reshape(NZ, 3, 4, 128), axes, split_axis=0, concat_axis=0, tiled=True
    )
    return pl.pallas_call(
        finish_kernel,
        out_shape=jax.ShapeDtypeStruct((4, 1, NY, NX), f32),
        in_specs=[VMEM] * 5,
        out_specs=VMEM,
        name="finish",
    )(back.reshape(NZ * ROWS_OUT, 128), side, LAST, SECOND_BACK, UNTWIST)


def solution(mesh):
    in_specs = (
        P(None, ("px", "py"), None, None),
        P(None, ("px", "py"), None, None),
        P(("px", "py")),
        P(("px", "py")),
        P(),
        P(),
    )
    out_specs = P(None, ("px", "py"), None, None)
    return jax.shard_map(local, mesh=mesh, in_specs=in_specs, out_specs=out_specs, check_vma=False)
```

```python
import math

import jax
import jax.numpy as jnp
import numpy as np
from jax import lax
from jax.experimental import pallas as pl
from jax.experimental.pallas import tpu as pltpu
from jax.sharding import PartitionSpec as P

SUBSTEPS = 8
NX, NY, NZ = 4096, 16, 128
N1, N2 = 32, 128
HN = N1 // 2
KAP = NY // 2
HALF = 0.275
FAST = 1.0 / SUBSTEPS
NOW = (-1.0, 2.0, 0.5, 1.5)
PAST = (1.0, -0.5, 0.25, -1.0)
CHUNKS = ((0, 1),)

f32 = jnp.float32
bf16 = jnp.bfloat16


def thrice(table):
    high = np.asarray(jnp.asarray(table, f32).astype(bf16))
    low = np.asarray(jnp.asarray(np.asarray(table, np.float64) - high.astype(np.float64), bf16))
    return np.concatenate([high, low, high], axis=-1)


def tables():
    y = np.arange(NY)
    kap = np.arange(KAP)
    qa = np.cos(2 * np.pi * kap[:, None] * y[None, :] / NY) * math.sqrt(2.0 / NY)
    qb = np.sin(2 * np.pi * kap[:, None] * y[None, :] / NY) * math.sqrt(2.0 / NY)
    qa[0] = 1.0 / math.sqrt(NY)
    qb[0] = (-1.0) ** y / math.sqrt(NY)
    q = qa + 1j * qb
    n1 = np.arange(HN)
    n2 = np.arange(N2)
    firsts, lasts, twists, untwists = [], [], [], []
    for parity in range(2):
        k1 = 2 * np.arange(HN) + parity
        dft1 = np.exp(-2j * np.pi * (k1[:, None] * n1[None, :] % N1) / N1)
        stage = np.einsum("kn,cy->kcny", dft1, q).reshape(HN, KAP, HN, 2, 8)
        stage = stage.transpose(0, 1, 3, 2, 4).reshape(HN * KAP, 2 * HN * 8)
        first = np.concatenate([stage.real, stage.imag], 0)
        firsts.append(thrice(first))
        lasts.append(thrice(first.T / NX))
        turn = 2 * np.pi * (k1[:, None] * n2[None, :]) / NX
        twists.append(np.stack([np.cos(turn), np.sin(turn)]))
        wide = np.repeat(turn.T, KAP, axis=1)
        untwists.append(np.stack([np.cos(wide), np.sin(wide)]))
    angle = 2 * np.pi * (n2[:, None] * n2[None, :] % N2) / N2
    cos, sin = np.cos(angle), np.sin(angle)
    second = np.block([[cos, sin], [-sin, cos]])
    return (
        np.stack(firsts),
        np.stack(lasts),
        thrice(second),
        thrice(second.T),
        np.stack(twists).astype(np.float32),
        np.stack(untwists).astype(np.float32),
    )


FIRST, LAST, SECOND, SECOND_BACK, TWIST, UNTWIST = tables()


def stacked(value, axis):
    high = value.astype(bf16)
    low = (value - high.astype(f32)).astype(bf16)
    return jnp.concatenate([high, high, low], axis=axis)


def product(left, right):
    return lax.dot_general(left, stacked(right, 0), (((1,), (0,)), ((), ())), preferred_element_type=f32)


def product_across(left, right):
    return lax.dot_general(left, stacked(right, 1), (((1,), (1,)), ((), ())), preferred_element_type=f32)


def butterfly(plane, parity):
    parts = []
    for b in range(2):
        rows = slice(8 * b, 8 * b + 8)
        for n in range(HN):
            near = plane[rows, N2 * n : N2 * n + N2]
            far = plane[rows, N2 * (n + HN) : N2 * (n + HN) + N2]
            parts.append(near - far if parity else near + far)
    return jnp.concatenate(parts, axis=0)


def forward(planes, parity, first, second, twist):
    columns = jnp.concatenate([butterfly(plane, parity) for plane in planes], axis=1)
    mid = product(first[parity], columns)
    turned = []
    for index in range(2):
        at = slice(N2 * index, N2 * index + N2)
        real, imag = [], []
        for m in range(HN):
            zr, zi = mid[8 * m : 8 * m + 8, at], mid[128 + 8 * m : 128 + 8 * m + 8, at]
            c, s = twist[parity, 0, m : m + 1, :], twist[parity, 1, m : m + 1, :]
            real.append(zr * c + zi * s)
            imag.append(zi * c - zr * s)
        turned.append(jnp.concatenate([jnp.concatenate(real, 0), jnp.concatenate(imag, 0)], axis=1))
    return product_across(second[...], jnp.concatenate(turned, axis=0))


def backward(modes, last, second_back, untwist):
    sides = []
    for parity in range(2):
        mid = product(second_back[...], modes[parity])
        turned = []
        for index in range(mid.shape[1] // 128):
            at = slice(128 * index, 128 * index + 128)
            zr, zi = mid[:N2, at], mid[N2:, at]
            c, s = untwist[parity, 0], untwist[parity, 1]
            turned.append(jnp.concatenate([zr * c - zi * s, zr * s + zi * c], axis=1))
        sides.append(product_across(last[parity], jnp.concatenate(turned, axis=0)))
    return sides


def real_tiles(sides, index):
    at = slice(128 * index, 128 * index + 128)
    for b in range(2):
        for n in range(HN):
            here = slice(8 * (b * HN + n), 8 * (b * HN + n) + 8)
            even, odd = sides[0][here, at], sides[1][here, at]
            rows = slice(8 * b, 8 * b + 8)
            yield rows, slice(N2 * n, N2 * n + N2), even + odd
            yield rows, slice(N2 * (n + HN), N2 * (n + HN) + N2), even - odd


def diff_x(plane):
    return pltpu.roll(plane, NX - 1, 1) - pltpu.roll(plane, 1, 1)


def diff_y(plane):
    return pltpu.roll(plane, NY - 1, 0) - pltpu.roll(plane, 1, 0)


def rows_in(parities):
    return 12 * len(parities) + (1 if 0 in parities else 0)


def rows_out(parities):
    return 6 * len(parities)


def row_in(parities, which, index, parity, part):
    return 12 * parities.index(parity) + 6 * which + 2 * index + part


def row_out(parities, index, parity, part):
    return 6 * parities.index(parity) + 2 * index + part


def send_kernel(parities, wind, damping, state, past, first, second, twist, out, here, then, one, two, tw, sems):
    copies = {}
    order = [("one", first, one), ("s2", state.at[2, 0], here.at[2]), ("s3", state.at[3, 0], here.at[3])]
    order += [("tw", twist, tw), ("two", second, two)]
    order += [("p2", past.at[2, 0], then.at[2]), ("p3", past.at[3, 0], then.at[3])]
    order += [("s0", state.at[0, 0], here.at[0]), ("s1", state.at[1, 0], here.at[1])]
    order += [("p0", past.at[0, 0], then.at[0]), ("p1", past.at[1, 0], then.at[1])]
    for number, (name, source, target) in enumerate(order):
        copies[name] = pltpu.make_async_copy(source, target, sems.at[number])
        copies[name].start()
    stride = rows_in(parities)

    def emit(pair, planes):
        for parity in parities:
            modes = forward(planes, parity, one, two, tw)
            for slot, (which, index) in enumerate(pair):
                for part in range(2):
                    block = modes[N2 * part : N2 * part + N2, 128 * slot : 128 * slot + 128]
                    out[pl.ds(row_in(parities, which, index, parity, part), N2, stride=stride), :] = block

    if 0 in parities:
        lane = lax.broadcasted_iota(jnp.int32, (N2, 128), 1)
        out[pl.ds(stride - 1, N2, stride=stride), :] = jnp.where(lane < 64, damping[0], wind[0])
    for name in ("one", "s2", "s3", "tw", "two"):
        copies[name].wait()
    emit(((0, 1), (0, 2)), (here[2], here[3]))
    for name in ("p2", "p3"):
        copies[name].wait()
    emit(((1, 1), (1, 2)), (then[2], then[3]))
    for name in ("s0", "s1", "p0", "p1"):
        copies[name].wait()
    emit(((0, 0), (1, 0)), (diff_x(here[0]) + diff_y(here[1]), diff_x(then[0]) + diff_y(then[1])))


def weight(section, table, step):
    row = section[step]
    value = jnp.where(row == 3, table[3], 0.0)
    for entry in range(3):
        value = jnp.where(row == entry, table[entry], value)
    return value


def local_kernel(wind, damping, section, state, past, first, last, second, second_back, twist, untwist, out):
    total_now = weight(section, NOW, 0)
    total_past = weight(section, PAST, 0)
    for step in range(1, SUBSTEPS):
        total_now = total_now + weight(section, NOW, step)
        total_past = total_past + weight(section, PAST, step)
    scaled = []
    for parity in range(2):
        lane = lax.broadcasted_iota(jnp.int32, (N2, 256), 1) % 128
        k = lax.broadcasted_iota(jnp.int32, (N2, 256), 0) * N1 + 2 * (lane // KAP) + parity
        fold = jnp.minimum(k, NX - k).astype(f32) * (2.0 / NX)
        fold = fold * fold
        signed = jnp.where(k > NX // 2, k - NX, k)
        signed = jnp.where(k == NX // 2, 0, signed).astype(f32) * (2.0 * math.pi / NX)
        damp = (fold * fold) * (damping[0] * -1.0)
        drift = signed * wind[0]
        modes = forward((state[0, 0], state[1, 0]), parity, first, second, twist)
        fr, fi = modes[:N2], modes[N2:]
        scaled.append(jnp.concatenate([damp * fr + drift * fi, damp * fi - drift * fr], axis=0))
    sides = backward(scaled, last, second_back, untwist)
    for index in range(2):
        for rows, cols, slow in real_tiles(sides, index):
            out[index, rows, cols] = state[index, 0, rows, cols] + FAST * (
                total_now * slow + total_past * past[index, 0, rows, cols]
            )


def lane_tables(index, parity):
    lane = lax.broadcasted_iota(jnp.int32, (8, 128), 1)
    k = index * N1 + 2 * (lane // KAP) + parity
    fold = jnp.minimum(k, NX - k).astype(f32) * (2.0 / NX)
    fold = fold * fold
    signed = jnp.where(k > NX // 2, k - NX, k)
    signed = jnp.where(k == NX // 2, 0, signed).astype(f32) * (2.0 * math.pi / NX)
    sx = jnp.sin(k.astype(f32) * (2.0 * math.pi / NX))
    sy = jnp.sin((lane % KAP).astype(f32) * (2.0 * math.pi / NY))
    coupling = (4.0 * HALF) * (sx * sx + sy * sy)
    return (fold * fold)[0:1], signed[0:1], coupling[0:1]


def column_kernel(parities, section, index, inverse, *refs):
    params, (got, out, chi, slow, up, press, total, inv_here, sem) = refs[0], refs[-9:]
    fetch = pltpu.make_async_copy(inverse, inv_here, sem)
    fetch.start()
    lanes = {parity: lane_tables(index[0], parity) for parity in parities}
    zero = jnp.zeros((8, 128), f32)
    stride, stride_out = rows_in(parities), rows_out(parities)
    first_stride = rows_in(CHUNKS[0])
    level = params[pl.ds(first_stride - 1, NZ, stride=first_stride), :]
    damping, wind = level[:, 0:1], level[:, 64:65]
    slots = [(parity, part) for parity in parities for part in range(2)]

    def plane(which, index, slot):
        return got[pl.ds(row_in(parities, which, index, *slot), NZ, stride=stride), :]

    for place in range(0, len(slots), 2):
        parity = slots[place][0]
        damp = -damping * lanes[parity][0]
        drift = wind * lanes[parity][1]
        for index in range(3):
            fr, fi = plane(0, index, slots[place]), plane(0, index, slots[place + 1])
            slow[index, place] = damp * fr + drift * fi
            slow[index, place + 1] = damp * fi - drift * fr
            if index == 0:
                chi[place] = fr
                chi[place + 1] = fi
    fetch.wait()
    high = inv_here[...].astype(bf16)
    low = (inv_here[...] - high.astype(f32)).astype(bf16)
    inv = jnp.concatenate([high, low, high], axis=1)
    upright = jnp.concatenate(
        [jnp.concatenate([plane(0, index, slot) for slot in slots], axis=1) for index in (1, 2)], axis=0
    )
    solved = product(inv, upright)
    for place in range(len(slots)):
        up[place, 8 : 8 + NZ] = solved[:NZ, 128 * place : 128 * place + 128]
        press[place, 8 : 8 + NZ] = solved[NZ:, 128 * place : 128 * place + 128]
        total[place] = jnp.zeros((NZ, 128), f32)
        for ref in (up, press):
            ref[place, 0:8] = zero
            ref[place, 8 + NZ : 16 + NZ] = zero

    def step_body(step, carry):
        now = weight(section, NOW, step) * FAST
        then = weight(section, PAST, step) * FAST
        for place, slot in enumerate(slots):
            coupling = lanes[slot[0]][2]
            p = press[place, 8 : 8 + NZ]
            fresh = chi[place] + coupling * p + (now * slow[0, place] + then * plane(1, 0, slot))
            chi[place] = fresh
            total[place] = total[place] + p
            up[place, 8 : 8 + NZ] = (
                up[place, 8 : 8 + NZ]
                - HALF * (press[place, 9 : 9 + NZ] - press[place, 7 : 7 + NZ])
                + (now * slow[1, place] + then * plane(1, 1, slot))
            )
            press[place, 8 : 8 + NZ] = (
                p
                - HALF * (fresh + (up[place, 9 : 9 + NZ] - up[place, 7 : 7 + NZ]))
                + (now * slow[2, place] + then * plane(1, 2, slot))
            )
        return carry

    lax.fori_loop(0, SUBSTEPS, step_body, 0)
    for place, slot in enumerate(slots):
        out[pl.ds(row_out(parities, 0, *slot), NZ, stride=stride_out), :] = total[place]
        out[pl.ds(row_out(parities, 1, *slot), NZ, stride=stride_out), :] = up[place, 8 : 8 + NZ]
        out[pl.ds(row_out(parities, 2, *slot), NZ, stride=stride_out), :] = press[place, 8 : 8 + NZ]


def finish_kernel(*refs):
    got = refs[: len(CHUNKS)]
    side, last, second_back, untwist, out, done, plane, sems = refs[len(CHUNKS) :]

    def modes_of(indices):
        modes = []
        for parity in range(2):
            (chunk,) = [c for c, parities in enumerate(CHUNKS) if parity in parities]
            parities = CHUNKS[chunk]
            cols = [
                jnp.concatenate(
                    [
                        got[chunk][pl.ds(row_out(parities, index, parity, part), N2, stride=rows_out(parities)), :]
                        for part in range(2)
                    ],
                    axis=0,
                )
                for index in indices
            ]
            modes.append(jnp.concatenate(cols, axis=1) if len(cols) > 1 else cols[0])
        return modes

    copies = [pltpu.make_async_copy(done.at[c], out.at[c, 0], sems.at[c]) for c in range(4)]
    sides = backward(modes_of((1, 2)), last, second_back, untwist)
    for index in range(2):
        for rows, cols, value in real_tiles(sides, index):
            done[2 + index, rows, cols] = value
        copies[2 + index].start()
    for rows, cols, value in real_tiles(backward(modes_of((0,)), last, second_back, untwist), 0):
        plane[rows, cols] = value
    done[1] = side[1] - HALF * diff_y(plane[...])
    copies[1].start()
    done[0] = side[0] - HALF * diff_x(plane[...])
    copies[0].start()
    for copy in copies:
        copy.wait()


VMEM = pl.BlockSpec(memory_space=pltpu.VMEM)
SMEM = pl.BlockSpec(memory_space=pltpu.SMEM)
ANY = pl.BlockSpec(memory_space=pl.ANY)


def near(array):
    return pltpu.with_memory_space_constraint(array, pltpu.VMEM)


def local(state, past_slow, mean_wind, damping, vertical_inverse, section):
    axes = ("px", "py")
    arrived = []
    for parities in CHUNKS:
        rows = rows_in(parities)
        message = pl.pallas_call(
            lambda *refs, parities=parities: send_kernel(parities, *refs),
            out_shape=pltpu.VMEM((NZ * rows, 128), f32),
            in_specs=[SMEM, SMEM] + [ANY] * 5,
            out_specs=VMEM,
            scratch_shapes=[
                pltpu.VMEM((4, NY, NX), f32),
                pltpu.VMEM((4, NY, NX), f32),
                pltpu.VMEM(FIRST.shape, bf16),
                pltpu.VMEM(SECOND.shape, bf16),
                pltpu.VMEM(TWIST.shape, f32),
                pltpu.SemaphoreType.DMA((11,)),
            ],
            name="send",
        )(mean_wind, damping, state, past_slow, FIRST, SECOND, TWIST)
        moved = lax.all_to_all(message.reshape(NZ, rows, 1, 128), axes, split_axis=0, concat_axis=0, tiled=True)
        arrived.append(near(moved.reshape(NZ * rows, 128)))
    side = pl.pallas_call(
        local_kernel,
        out_shape=pltpu.VMEM((2, NY, NX), f32),
        in_specs=[SMEM, SMEM, SMEM] + [VMEM] * 8,
        out_specs=VMEM,
        cost_estimate=pl.CostEstimate(flops=8_000_000_000, bytes_accessed=4_000_000, transcendentals=0),
        name="side",
    )(mean_wind, damping, section, state, past_slow, FIRST, LAST, SECOND, SECOND_BACK, TWIST, UNTWIST)
    place = lax.axis_index(axes).astype(jnp.int32).reshape(1)
    returned = []
    for chunk, parities in enumerate(CHUNKS):
        slots, rows = 2 * len(parities), rows_out(parities)
        padded = pltpu.VMEM((slots, NZ + 16, 128), f32)
        solved = pl.pallas_call(
            lambda *refs, parities=parities: column_kernel(parities, *refs),
            out_shape=pltpu.VMEM((NZ * rows, 128), f32),
            in_specs=[SMEM, SMEM, ANY] + [VMEM] * (1 + chunk),
            out_specs=VMEM,
            scratch_shapes=[
                pltpu.VMEM((slots, NZ, 128), f32),
                pltpu.VMEM((3, slots, NZ, 128), f32),
                padded,
                padded,
                pltpu.VMEM((slots, NZ, 128), f32),
                pltpu.VMEM((2 * NZ, 2 * NZ), f32),
                pltpu.SemaphoreType.DMA,
            ],
            name="columns",
        )(section, place, vertical_inverse, *arrived[: chunk + 1])
        back = lax.all_to_all(
            solved.reshape(NZ, rows // 2, 2, 128), axes, split_axis=0, concat_axis=0, tiled=True
        )
        returned.append(near(back.reshape(NZ * rows, 128)))
    return pl.pallas_call(
        finish_kernel,
        out_shape=jax.ShapeDtypeStruct((4, 1, NY, NX), f32),
        in_specs=[VMEM] * (len(CHUNKS) + 4),
        out_specs=ANY,
        scratch_shapes=[
            pltpu.VMEM((4, NY, NX), f32),
            pltpu.VMEM((NY, NX), f32),
            pltpu.SemaphoreType.DMA((4,)),
        ],
        name="finish",
    )(*returned, near(side), near(LAST), near(SECOND_BACK), near(UNTWIST))


def solution(mesh):
    in_specs = (
        P(None, ("px", "py"), None, None),
        P(None, ("px", "py"), None, None),
        P(("px", "py")),
        P(("px", "py")),
        P(),
        P(),
    )
    out_specs = P(None, ("px", "py"), None, None)
    return jax.shard_map(local, mesh=mesh, in_specs=in_specs, out_specs=out_specs, check_vma=False)
```

```python
import math

import jax
import jax.numpy as jnp
import numpy as np
from jax import lax
from jax.experimental import pallas as pl
from jax.experimental.pallas import tpu as pltpu
from jax.sharding import PartitionSpec as P

SUBSTEPS = 8
NX, NY, NZ = 4096, 16, 128
N1, N2 = 32, 128
HN = N1 // 2
KAP = NY // 2
HALF = 0.275
FAST = 1.0 / SUBSTEPS
NOW = (-1.0, 2.0, 0.5, 1.5)
PAST = (1.0, -0.5, 0.25, -1.0)
BOTH = (0, 1)

f32 = jnp.float32
bf16 = jnp.bfloat16


def thrice(table):
    high = np.asarray(jnp.asarray(table, f32).astype(bf16))
    low = np.asarray(jnp.asarray(np.asarray(table, np.float64) - high.astype(np.float64), bf16))
    return np.concatenate([high, low, high], axis=-1)


def tables():
    y = np.arange(NY)
    kap = np.arange(KAP)
    qa = np.cos(2 * np.pi * kap[:, None] * y[None, :] / NY) * math.sqrt(2.0 / NY)
    qb = np.sin(2 * np.pi * kap[:, None] * y[None, :] / NY) * math.sqrt(2.0 / NY)
    qa[0] = 1.0 / math.sqrt(NY)
    qb[0] = (-1.0) ** y / math.sqrt(NY)
    q = qa + 1j * qb
    n1 = np.arange(HN)
    n2 = np.arange(N2)
    firsts, lasts, twists, untwists = [], [], [], []
    for parity in range(2):
        k1 = 2 * np.arange(HN) + parity
        dft1 = np.exp(-2j * np.pi * (k1[:, None] * n1[None, :] % N1) / N1)
        stage = np.einsum("kn,cy->kcny", dft1, q).reshape(HN, KAP, HN, 2, 8)
        stage = stage.transpose(0, 1, 3, 2, 4).reshape(HN * KAP, 2 * HN * 8)
        first = np.concatenate([stage.real, stage.imag], 0)
        firsts.append(thrice(first))
        lasts.append(thrice(first.T / NX))
        turn = 2 * np.pi * (k1[:, None] * n2[None, :]) / NX
        twists.append(np.stack([np.cos(turn), np.sin(turn)]))
        wide = np.repeat(turn.T, KAP, axis=1)
        untwists.append(np.stack([np.cos(wide), np.sin(wide)]))
    angle = 2 * np.pi * (n2[:, None] * n2[None, :] % N2) / N2
    cos, sin = np.cos(angle), np.sin(angle)
    second = np.block([[cos, sin], [-sin, cos]])
    k2 = np.arange(N2)
    slopes = []
    for parity in range(2):
        k1 = np.repeat(2 * np.arange(HN) + parity, KAP)
        slopes.append(2 * np.sin(2 * np.pi * (k1[None, :] + N1 * k2[:, None]) / NX))
    across = np.tile(2 * np.sin(2 * np.pi * kap / NY), HN)
    return (
        np.stack(firsts),
        np.stack(lasts),
        thrice(second),
        thrice(second.T),
        np.stack(twists).astype(np.float32),
        np.stack(untwists).astype(np.float32),
        np.stack(slopes).astype(np.float32),
        np.tile(across, (8, 1)).astype(np.float32),
    )


FIRST, LAST, SECOND, SECOND_BACK, TWIST, UNTWIST, SLOPE, ACROSS = tables()


def stacked(value, axis):
    high = value.astype(bf16)
    low = (value - high.astype(f32)).astype(bf16)
    return jnp.concatenate([high, high, low], axis=axis)


def product(left, right):
    return lax.dot_general(left, stacked(right, 0), (((1,), (0,)), ((), ())), preferred_element_type=f32)


def product_across(left, right):
    return lax.dot_general(left, stacked(right, 1), (((1,), (1,)), ((), ())), preferred_element_type=f32)


def butterfly(plane, parity):
    parts = []
    for b in range(2):
        rows = slice(8 * b, 8 * b + 8)
        for n in range(HN):
            near = plane[rows, N2 * n : N2 * n + N2]
            far = plane[rows, N2 * (n + HN) : N2 * (n + HN) + N2]
            parts.append(near - far if parity else near + far)
    return jnp.concatenate(parts, axis=0)


def forward(planes, parity, first, second, twist):
    columns = jnp.concatenate([butterfly(plane, parity) for plane in planes], axis=1)
    mid = product(first[parity], columns)
    turned = []
    for index in range(2):
        at = slice(N2 * index, N2 * index + N2)
        real, imag = [], []
        for m in range(HN):
            zr, zi = mid[8 * m : 8 * m + 8, at], mid[128 + 8 * m : 128 + 8 * m + 8, at]
            c, s = twist[parity, 0, m : m + 1, :], twist[parity, 1, m : m + 1, :]
            real.append(zr * c + zi * s)
            imag.append(zi * c - zr * s)
        turned.append(jnp.concatenate([jnp.concatenate(real, 0), jnp.concatenate(imag, 0)], axis=1))
    return product_across(second[...], jnp.concatenate(turned, axis=0))


def backward(modes, last, second_back, untwist):
    sides = []
    for parity in range(2):
        mid = product(second_back[...], modes[parity])
        turned = []
        for index in range(mid.shape[1] // 128):
            at = slice(128 * index, 128 * index + 128)
            zr, zi = mid[:N2, at], mid[N2:, at]
            c, s = untwist[parity, 0], untwist[parity, 1]
            turned.append(jnp.concatenate([zr * c - zi * s, zr * s + zi * c], axis=1))
        sides.append(product_across(last[parity], jnp.concatenate(turned, axis=0)))
    return sides


def real_tiles(sides, index):
    at = slice(128 * index, 128 * index + 128)
    for b in range(2):
        for n in range(HN):
            here = slice(8 * (b * HN + n), 8 * (b * HN + n) + 8)
            even, odd = sides[0][here, at], sides[1][here, at]
            rows = slice(8 * b, 8 * b + 8)
            yield rows, slice(N2 * n, N2 * n + N2), even + odd
            yield rows, slice(N2 * (n + HN), N2 * (n + HN) + N2), even - odd


def rows_in(parities):
    return 12 * len(parities) + (1 if 0 in parities else 0)


def rows_out(parities):
    return 6 * len(parities)


def row_in(parities, which, index, parity, part):
    return 12 * parities.index(parity) + 6 * which + 2 * index + part


def row_out(parities, index, parity, part):
    return 6 * parities.index(parity) + 2 * index + part


def weight(section, table, step):
    row = section[step]
    value = jnp.where(row == 3, table[3], 0.0)
    for entry in range(3):
        value = jnp.where(row == entry, table[entry], value)
    return value


def times_i(slope, value):
    return jnp.concatenate([-slope * value[N2:], slope * value[:N2]], axis=0)


def send_kernel(
    wind, damping, section, state, past, first, second, twist, slope, across, out, kept, here, then, one, two, tw, sl, ac, sems
):
    copies = {}
    order = [("one", first, one), ("s2", state.at[2, 0], here.at[2]), ("s3", state.at[3, 0], here.at[3])]
    order += [("tw", twist, tw), ("two", second, two)]
    order += [("p2", past.at[2, 0], then.at[2]), ("p3", past.at[3, 0], then.at[3])]
    order += [("s0", state.at[0, 0], here.at[0]), ("s1", state.at[1, 0], here.at[1])]
    order += [("sl", slope, sl), ("ac", across, ac)]
    order += [("p0", past.at[0, 0], then.at[0]), ("p1", past.at[1, 0], then.at[1])]
    for number, (name, source, target) in enumerate(order):
        copies[name] = pltpu.make_async_copy(source, target, sems.at[number])
        copies[name].start()
    stride = rows_in(BOTH)

    def put(which, index, parity, modes):
        for part in range(2):
            rows = pl.ds(row_in(BOTH, which, index, parity, part), N2, stride=stride)
            out[rows, :] = modes[N2 * part : N2 * part + N2]

    lane = lax.broadcasted_iota(jnp.int32, (N2, 128), 1)
    out[pl.ds(stride - 1, N2, stride=stride), :] = jnp.where(lane < 64, damping[0], wind[0])
    total_now = weight(section, NOW, 0)
    total_past = weight(section, PAST, 0)
    for step in range(1, SUBSTEPS):
        total_now = total_now + weight(section, NOW, step)
        total_past = total_past + weight(section, PAST, step)
    total_now = total_now * FAST
    total_past = total_past * FAST
    for name in ("one", "s2", "s3", "tw", "two"):
        copies[name].wait()
    for parity in range(2):
        modes = forward((here[2], here[3]), parity, one, two, tw)
        put(0, 1, parity, modes[:, :128])
        put(0, 2, parity, modes[:, 128:])
    for name in ("p2", "p3"):
        copies[name].wait()
    for parity in range(2):
        modes = forward((then[2], then[3]), parity, one, two, tw)
        put(1, 1, parity, modes[:, :128])
        put(1, 2, parity, modes[:, 128:])
    for name in ("s0", "s1", "sl", "ac", "p0", "p1"):
        copies[name].wait()
    for parity in range(2):
        modes = forward((here[0], here[1]), parity, one, two, tw)
        earlier = forward((then[0], then[1]), parity, one, two, tw)
        steep, aside = sl[parity], ac[0:1]
        put(0, 0, parity, times_i(steep, modes[:, :128]) - times_i(aside, modes[:, 128:]))
        put(1, 0, parity, times_i(steep, earlier[:, :128]) - times_i(aside, earlier[:, 128:]))
        k = lax.broadcasted_iota(jnp.int32, (N2, 128), 0) * N1 + 2 * (lane // KAP) + parity
        fold = jnp.minimum(k, NX - k).astype(f32) * (2.0 / NX)
        fold = fold * fold
        signed = jnp.where(k > NX // 2, k - NX, k)
        signed = jnp.where(k == NX // 2, 0, signed).astype(f32) * (2.0 * math.pi / NX)
        keep = 1.0 - (fold * fold) * (damping[0] * total_now)
        drift = signed * (wind[0] * total_now)
        for index in range(2):
            at = slice(128 * index, 128 * index + 128)
            fr, fi = modes[:N2, at], modes[N2:, at]
            kept[parity, :N2, at] = (keep * fr + drift * fi) + total_past * earlier[:N2, at]
            kept[parity, N2:, at] = (keep * fi - drift * fr) + total_past * earlier[N2:, at]


def lane_tables(index, parity):
    lane = lax.broadcasted_iota(jnp.int32, (8, 128), 1)
    k = index * N1 + 2 * (lane // KAP) + parity
    fold = jnp.minimum(k, NX - k).astype(f32) * (2.0 / NX)
    fold = fold * fold
    signed = jnp.where(k > NX // 2, k - NX, k)
    signed = jnp.where(k == NX // 2, 0, signed).astype(f32) * (2.0 * math.pi / NX)
    sx = jnp.sin(k.astype(f32) * (2.0 * math.pi / NX))
    sy = jnp.sin((lane % KAP).astype(f32) * (2.0 * math.pi / NY))
    coupling = (4.0 * HALF) * (sx * sx + sy * sy)
    return (fold * fold)[0:1], signed[0:1], coupling[0:1]


def column_kernel(parities, section, inverse, *refs):
    params, (got, out, chi, slow, up, press, total) = refs[0], refs[-7:]
    lanes = {parity: lane_tables(lax.axis_index(("px", "py")), parity) for parity in parities}
    zero = jnp.zeros((8, 128), f32)
    stride, stride_out = rows_in(parities), rows_out(parities)
    first_stride = rows_in(BOTH)
    level = params[pl.ds(first_stride - 1, NZ, stride=first_stride), :]
    damping, wind = level[:, 0:1], level[:, 64:65]
    slots = [(parity, part) for parity in parities for part in range(2)]

    def plane(which, index, slot):
        return got[pl.ds(row_in(parities, which, index, *slot), NZ, stride=stride), :]

    for place in range(0, len(slots), 2):
        parity = slots[place][0]
        damp = -damping * lanes[parity][0]
        drift = wind * lanes[parity][1]
        for index in range(3):
            fr, fi = plane(0, index, slots[place]), plane(0, index, slots[place + 1])
            slow[index, place] = damp * fr + drift * fi
            slow[index, place + 1] = damp * fi - drift * fr
            if index == 0:
                chi[place] = fr
                chi[place + 1] = fi
    high = inverse[...].astype(bf16)
    low = (inverse[...] - high.astype(f32)).astype(bf16)
    inv = jnp.concatenate([high, low, high], axis=1)
    upright = jnp.concatenate(
        [jnp.concatenate([plane(0, index, slot) for slot in slots], axis=1) for index in (1, 2)], axis=0
    )
    solved = product(inv, upright)
    for place in range(len(slots)):
        up[place, 8 : 8 + NZ] = solved[:NZ, 128 * place : 128 * place + 128]
        press[place, 8 : 8 + NZ] = solved[NZ:, 128 * place : 128 * place + 128]
        total[place] = jnp.zeros((NZ, 128), f32)
        for ref in (up, press):
            ref[place, 0:8] = zero
            ref[place, 8 + NZ : 16 + NZ] = zero

    def step_body(step, carry):
        now = weight(section, NOW, step) * FAST
        then = weight(section, PAST, step) * FAST
        for place, slot in enumerate(slots):
            coupling = lanes[slot[0]][2]
            p = press[place, 8 : 8 + NZ]
            fresh = chi[place] + coupling * p + (now * slow[0, place] + then * plane(1, 0, slot))
            chi[place] = fresh
            total[place] = total[place] + p
            up[place, 8 : 8 + NZ] = (
                up[place, 8 : 8 + NZ]
                - HALF * (press[place, 9 : 9 + NZ] - press[place, 7 : 7 + NZ])
                + (now * slow[1, place] + then * plane(1, 1, slot))
            )
            press[place, 8 : 8 + NZ] = (
                p
                - HALF * (fresh + (up[place, 9 : 9 + NZ] - up[place, 7 : 7 + NZ]))
                + (now * slow[2, place] + then * plane(1, 2, slot))
            )
        return carry

    lax.fori_loop(0, SUBSTEPS, step_body, 0)
    for place, slot in enumerate(slots):
        out[pl.ds(row_out(parities, 0, *slot), NZ, stride=stride_out), :] = total[place]
        out[pl.ds(row_out(parities, 1, *slot), NZ, stride=stride_out), :] = up[place, 8 : 8 + NZ]
        out[pl.ds(row_out(parities, 2, *slot), NZ, stride=stride_out), :] = press[place, 8 : 8 + NZ]


def finish_kernel(got, kept, last, second_back, untwist, slope, across, out, done, sems):
    def modes_of(index, parity):
        rows = [pl.ds(row_out(BOTH, index, parity, part), N2, stride=rows_out(BOTH)) for part in range(2)]
        return jnp.concatenate([got[rows[0], :], got[rows[1], :]], axis=0)

    copies = [pltpu.make_async_copy(done.at[c], out.at[c, 0], sems.at[c]) for c in range(4)]

    def finish(modes, base):
        sides = backward(modes, last, second_back, untwist)
        for index in range(2):
            for rows, cols, value in real_tiles(sides, index):
                done[base + index, rows, cols] = value
            copies[base + index].start()

    finish([jnp.concatenate([modes_of(1, q), modes_of(2, q)], axis=1) for q in BOTH], 2)
    flows = []
    for parity in BOTH:
        total = modes_of(0, parity)
        steep, aside = HALF * slope[parity], HALF * across[0:1]
        flows.append(
            jnp.concatenate(
                [kept[parity, :, :128] - times_i(steep, total), kept[parity, :, 128:] + times_i(aside, total)], axis=1
            )
        )
    finish(flows, 0)
    for copy in copies:
        copy.wait()


VMEM = pl.BlockSpec(memory_space=pltpu.VMEM)
SMEM = pl.BlockSpec(memory_space=pltpu.SMEM)
HBM = pl.BlockSpec(memory_space=pltpu.HBM)
ROOM = pltpu.CompilerParams(vmem_limit_bytes=40 * 2**20)


def near(array):
    return pltpu.with_memory_space_constraint(array, pltpu.VMEM)


def local(state, past_slow, mean_wind, damping, vertical_inverse, section):
    axes = ("px", "py")
    rows = rows_in(BOTH)
    message, kept = pl.pallas_call(
        send_kernel,
        out_shape=[pltpu.VMEM((NZ * rows, 128), f32), pltpu.VMEM((2, 2 * N2, 256), f32)],
        in_specs=[SMEM, SMEM, SMEM] + [HBM] * 7,
        out_specs=[VMEM, VMEM],
        scratch_shapes=[
            pltpu.VMEM((4, NY, NX), f32),
            pltpu.VMEM((4, NY, NX), f32),
            pltpu.VMEM(FIRST.shape, bf16),
            pltpu.VMEM(SECOND.shape, bf16),
            pltpu.VMEM(TWIST.shape, f32),
            pltpu.VMEM(SLOPE.shape, f32),
            pltpu.VMEM(ACROSS.shape, f32),
            pltpu.SemaphoreType.DMA((13,)),
        ],
        name="send",
    )(mean_wind, damping, section, state, past_slow, FIRST, SECOND, TWIST, SLOPE, ACROSS)
    moved = lax.all_to_all(message.reshape(NZ, rows, 1, 128), axes, split_axis=0, concat_axis=0, tiled=True)
    arrived = near(moved.reshape(NZ * rows, 128))
    rows = rows_out(BOTH)
    padded = pltpu.VMEM((4, NZ + 16, 128), f32)
    solved = pl.pallas_call(
        lambda *refs: column_kernel(BOTH, *refs),
        out_shape=pltpu.VMEM((NZ * rows, 128), f32),
        in_specs=[SMEM, VMEM, VMEM],
        out_specs=VMEM,
        scratch_shapes=[
            pltpu.VMEM((4, NZ, 128), f32),
            pltpu.VMEM((3, 4, NZ, 128), f32),
            padded,
            padded,
            pltpu.VMEM((4, NZ, 128), f32),
        ],
        compiler_params=ROOM,
        name="columns",
    )(section, near(vertical_inverse), arrived)
    back = lax.all_to_all(solved.reshape(NZ, rows // 2, 2, 128), axes, split_axis=0, concat_axis=0, tiled=True)
    returned = near(back.reshape(NZ * rows, 128))
    return pl.pallas_call(
        finish_kernel,
        out_shape=jax.ShapeDtypeStruct((4, 1, NY, NX), f32),
        in_specs=[VMEM] * 7,
        out_specs=HBM,
        scratch_shapes=[pltpu.VMEM((4, NY, NX), f32), pltpu.SemaphoreType.DMA((4,))],
        compiler_params=ROOM,
        name="finish",
    )(returned, near(kept), near(LAST), near(SECOND_BACK), near(UNTWIST), near(SLOPE), near(ACROSS))


def solution(mesh):
    in_specs = (
        P(None, ("px", "py"), None, None),
        P(None, ("px", "py"), None, None),
        P(("px", "py")),
        P(("px", "py")),
        P(),
        P(),
    )
    out_specs = P(None, ("px", "py"), None, None)
    return jax.shard_map(local, mesh=mesh, in_specs=in_specs, out_specs=out_specs, check_vma=False)
```

```python
import math

import jax
import jax.numpy as jnp
import numpy as np
from jax import lax
from jax.experimental import pallas as pl
from jax.experimental.pallas import tpu as pltpu
from jax.sharding import PartitionSpec as P

SUBSTEPS = 8
NX, NY, NZ = 4096, 16, 128
N1, N2 = 32, 128
HN = N1 // 2
KAP = NY // 2
HALF = 0.275
FAST = 1.0 / SUBSTEPS
NOW = (-1.0, 2.0, 0.5, 1.5)
PAST = (1.0, -0.5, 0.25, -1.0)
BOTH = (0, 1)

f32 = jnp.float32
bf16 = jnp.bfloat16


def halves(table):
    high = np.asarray(jnp.asarray(table, f32).astype(bf16))
    low = np.asarray(jnp.asarray(np.asarray(table, np.float64) - high.astype(np.float64), bf16))
    return np.concatenate([high, low], axis=-1)


def tables():
    y = np.arange(NY)
    kap = np.arange(KAP)
    qa = np.cos(2 * np.pi * kap[:, None] * y[None, :] / NY) * math.sqrt(2.0 / NY)
    qb = np.sin(2 * np.pi * kap[:, None] * y[None, :] / NY) * math.sqrt(2.0 / NY)
    qa[0] = 1.0 / math.sqrt(NY)
    qb[0] = (-1.0) ** y / math.sqrt(NY)
    q = qa + 1j * qb
    n1 = np.arange(HN)
    n2 = np.arange(N2)
    firsts, lasts, twists, untwists = [], [], [], []
    for parity in range(2):
        k1 = 2 * np.arange(HN) + parity
        dft1 = np.exp(-2j * np.pi * (k1[:, None] * n1[None, :] % N1) / N1)
        stage = np.einsum("kn,cy->kcny", dft1, q).reshape(HN, KAP, HN, 2, 8)
        stage = stage.transpose(0, 1, 3, 2, 4).reshape(HN * KAP, 2 * HN * 8)
        first = np.concatenate([stage.real, stage.imag], 0)
        firsts.append(halves(first))
        lasts.append(halves(first.T / NX))
        turn = 2 * np.pi * (k1[:, None] * n2[None, :]) / NX
        twists.append(np.stack([np.cos(turn), np.sin(turn)]))
        wide = np.repeat(turn.T, KAP, axis=1)
        untwists.append(np.stack([np.cos(wide), np.sin(wide)]))
    angle = 2 * np.pi * (n2[:, None] * n2[None, :] % N2) / N2
    cos, sin = np.cos(angle), np.sin(angle)
    second = np.block([[cos, sin], [-sin, cos]])
    k2 = np.arange(N2)
    slopes = []
    for parity in range(2):
        k1 = np.repeat(2 * np.arange(HN) + parity, KAP)
        slopes.append(2 * np.sin(2 * np.pi * (k1[None, :] + N1 * k2[:, None]) / NX))
    across = np.tile(2 * np.sin(2 * np.pi * kap / NY), HN)
    return (
        np.stack(firsts),
        np.stack(lasts),
        halves(second),
        halves(second.T),
        np.stack(twists).astype(np.float32),
        np.stack(untwists).astype(np.float32),
        np.stack(slopes).astype(np.float32),
        np.tile(across, (8, 1)).astype(np.float32),
    )


FIRST, LAST, SECOND, SECOND_BACK, TWIST, UNTWIST, SLOPE, ACROSS = tables()


def product(left, right, dims=((1,), (0,))):
    high = right.astype(bf16)
    low = (right - high.astype(f32)).astype(bf16)

    def dot(table, data):
        return lax.dot_general(table, data, (dims, ((), ())), preferred_element_type=f32)

    count = left.shape[0]
    both = dot(jnp.concatenate([left[:, :256], left[:, 256:]], axis=0), high)
    return both[:count] + (both[count:] + dot(left[:, :256], low))


def product_across(left, right):
    return product(left, right, ((1,), (1,)))


def butterfly(plane, parity):
    parts = []
    for b in range(2):
        rows = slice(8 * b, 8 * b + 8)
        for n in range(HN):
            near = plane[rows, N2 * n : N2 * n + N2]
            far = plane[rows, N2 * (n + HN) : N2 * (n + HN) + N2]
            parts.append(near - far if parity else near + far)
    return jnp.concatenate(parts, axis=0)


def forward(planes, parity, first, second, twist):
    columns = jnp.concatenate([butterfly(plane, parity) for plane in planes], axis=1)
    mid = product(first[parity], columns)
    turned = []
    for index in range(2):
        at = slice(N2 * index, N2 * index + N2)
        real, imag = [], []
        for m in range(HN):
            zr, zi = mid[8 * m : 8 * m + 8, at], mid[128 + 8 * m : 128 + 8 * m + 8, at]
            c, s = twist[parity, 0, m : m + 1, :], twist[parity, 1, m : m + 1, :]
            real.append(zr * c + zi * s)
            imag.append(zi * c - zr * s)
        turned.append(jnp.concatenate([jnp.concatenate(real, 0), jnp.concatenate(imag, 0)], axis=1))
    return product_across(second[...], jnp.concatenate(turned, axis=0))


def backward(modes, last, second_back, untwist):
    sides = []
    for parity in range(2):
        mid = product(second_back[...], modes[parity])
        turned = []
        for index in range(mid.shape[1] // 128):
            at = slice(128 * index, 128 * index + 128)
            zr, zi = mid[:N2, at], mid[N2:, at]
            c, s = untwist[parity, 0], untwist[parity, 1]
            turned.append(jnp.concatenate([zr * c - zi * s, zr * s + zi * c], axis=1))
        sides.append(product_across(last[parity], jnp.concatenate(turned, axis=0)))
    return sides


def real_tiles(sides, index):
    at = slice(128 * index, 128 * index + 128)
    for b in range(2):
        for n in range(HN):
            here = slice(8 * (b * HN + n), 8 * (b * HN + n) + 8)
            even, odd = sides[0][here, at], sides[1][here, at]
            rows = slice(8 * b, 8 * b + 8)
            yield rows, slice(N2 * n, N2 * n + N2), even + odd
            yield rows, slice(N2 * (n + HN), N2 * (n + HN) + N2), even - odd


def rows_in(parities):
    return 12 * len(parities) + (1 if 0 in parities else 0)


def rows_out(parities):
    return 6 * len(parities)


def row_in(parities, which, index, parity, part):
    return 12 * parities.index(parity) + 6 * which + 2 * index + part


def row_out(parities, index, parity, part):
    return 6 * parities.index(parity) + 2 * index + part


def weight(section, table, step):
    row = section[step]
    value = jnp.where(row == 3, table[3], 0.0)
    for entry in range(3):
        value = jnp.where(row == entry, table[entry], value)
    return value


def times_i(slope, value):
    return jnp.concatenate([-slope * value[N2:], slope * value[:N2]], axis=0)


def send_kernel(
    wind_in,
    damping_in,
    section_in,
    state,
    past,
    first,
    second,
    twist,
    slope,
    across,
    out,
    kept,
    here,
    then,
    one,
    two,
    tw,
    sl,
    ac,
    wind,
    damping,
    section,
    sems,
):
    copies = {}
    order = [("one", first, one), ("s2", state.at[2, 0], here.at[2]), ("s3", state.at[3, 0], here.at[3])]
    order += [("tw", twist, tw), ("two", second, two)]
    order += [("p2", past.at[2, 0], then.at[2]), ("p3", past.at[3, 0], then.at[3])]
    order += [("s0", state.at[0, 0], here.at[0]), ("s1", state.at[1, 0], here.at[1])]
    order += [("sl", slope, sl), ("ac", across, ac)]
    order += [("p0", past.at[0, 0], then.at[0]), ("p1", past.at[1, 0], then.at[1])]
    order += [("wind", wind_in, wind), ("damping", damping_in, damping), ("section", section_in, section)]
    for number, (name, source, target) in enumerate(order):
        copies[name] = pltpu.make_async_copy(source, target, sems.at[number])
        copies[name].start()
    stride = rows_in(BOTH)

    def put(which, index, parity, modes):
        for part in range(2):
            rows = pl.ds(row_in(BOTH, which, index, parity, part), N2, stride=stride)
            out[rows, :] = modes[N2 * part : N2 * part + N2]

    for name in copies:
        copies[name].wait()
    for parity in range(2):
        modes = forward((here[2], here[3]), parity, one, two, tw)
        put(0, 1, parity, modes[:, :128])
        put(0, 2, parity, modes[:, 128:])
    for parity in range(2):
        modes = forward((then[2], then[3]), parity, one, two, tw)
        put(1, 1, parity, modes[:, :128])
        put(1, 2, parity, modes[:, 128:])
    lane = lax.broadcasted_iota(jnp.int32, (N2, 128), 1)
    out[pl.ds(stride - 1, N2, stride=stride), :] = jnp.where(lane < 64, damping[0], wind[0])
    total_now = weight(section, NOW, 0)
    total_past = weight(section, PAST, 0)
    for step in range(1, SUBSTEPS):
        total_now = total_now + weight(section, NOW, step)
        total_past = total_past + weight(section, PAST, step)
    total_now = total_now * FAST
    total_past = total_past * FAST
    for parity in range(2):
        modes = forward((here[0], here[1]), parity, one, two, tw)
        earlier = forward((then[0], then[1]), parity, one, two, tw)
        steep, aside = sl[parity], ac[0:1]
        put(0, 0, parity, times_i(steep, modes[:, :128]) - times_i(aside, modes[:, 128:]))
        put(1, 0, parity, times_i(steep, earlier[:, :128]) - times_i(aside, earlier[:, 128:]))
        k = lax.broadcasted_iota(jnp.int32, (N2, 128), 0) * N1 + 2 * (lane // KAP) + parity
        fold = jnp.minimum(k, NX - k).astype(f32) * (2.0 / NX)
        fold = fold * fold
        signed = jnp.where(k > NX // 2, k - NX, k)
        signed = jnp.where(k == NX // 2, 0, signed).astype(f32) * (2.0 * math.pi / NX)
        keep = 1.0 - (fold * fold) * (damping[0] * total_now)
        drift = signed * (wind[0] * total_now)
        for index in range(2):
            at = slice(128 * index, 128 * index + 128)
            fr, fi = modes[:N2, at], modes[N2:, at]
            kept[parity, :N2, at] = (keep * fr + drift * fi) + total_past * earlier[:N2, at]
            kept[parity, N2:, at] = (keep * fi - drift * fr) + total_past * earlier[N2:, at]


def lane_tables(index, parity):
    lane = lax.broadcasted_iota(jnp.int32, (8, 128), 1)
    k = index * N1 + 2 * (lane // KAP) + parity
    fold = jnp.minimum(k, NX - k).astype(f32) * (2.0 / NX)
    fold = fold * fold
    signed = jnp.where(k > NX // 2, k - NX, k)
    signed = jnp.where(k == NX // 2, 0, signed).astype(f32) * (2.0 * math.pi / NX)
    sx = jnp.sin(k.astype(f32) * (2.0 * math.pi / NX))
    sy = jnp.sin((lane % KAP).astype(f32) * (2.0 * math.pi / NY))
    coupling = (4.0 * HALF) * (sx * sx + sy * sy)
    return (fold * fold)[0:1], signed[0:1], coupling[0:1]


def column_kernel(parities, section_in, inverse, got, out, chi, slow, up, press, total, section, sem):
    fetch = pltpu.make_async_copy(section_in, section, sem)
    fetch.start()
    lanes = {parity: lane_tables(lax.axis_index(("px", "py")), parity) for parity in parities}
    zero = jnp.zeros((8, 128), f32)
    stride, stride_out = rows_in(parities), rows_out(parities)
    first_stride = rows_in(BOTH)
    level = got[pl.ds(first_stride - 1, NZ, stride=first_stride), :]
    damping, wind = level[:, 0:1], level[:, 64:65]
    slots = [(parity, part) for parity in parities for part in range(2)]

    def plane(which, index, slot):
        return got[pl.ds(row_in(parities, which, index, *slot), NZ, stride=stride), :]

    for place in range(0, len(slots), 2):
        parity = slots[place][0]
        damp = -damping * lanes[parity][0]
        drift = wind * lanes[parity][1]
        for index in range(3):
            fr, fi = plane(0, index, slots[place]), plane(0, index, slots[place + 1])
            slow[index, place] = damp * fr + drift * fi
            slow[index, place + 1] = damp * fi - drift * fr
            if index == 0:
                chi[place] = fr
                chi[place + 1] = fi
    high = inverse[...].astype(bf16)
    low = (inverse[...] - high.astype(f32)).astype(bf16)
    inv = jnp.concatenate([high, low], axis=1)
    upright = jnp.concatenate(
        [jnp.concatenate([plane(0, index, slot) for slot in slots], axis=1) for index in (1, 2)], axis=0
    )
    solved = product(inv, upright)
    for place in range(len(slots)):
        up[place, 8 : 8 + NZ] = solved[:NZ, 128 * place : 128 * place + 128]
        press[place, 8 : 8 + NZ] = solved[NZ:, 128 * place : 128 * place + 128]
        total[place] = jnp.zeros((NZ, 128), f32)
        for ref in (up, press):
            ref[place, 0:8] = zero
            ref[place, 8 + NZ : 16 + NZ] = zero

    fetch.wait()

    def step_body(step, carry):
        now = weight(section, NOW, step) * FAST
        then = weight(section, PAST, step) * FAST
        for place, slot in enumerate(slots):
            coupling = lanes[slot[0]][2]
            p = press[place, 8 : 8 + NZ]
            fresh = chi[place] + coupling * p + (now * slow[0, place] + then * plane(1, 0, slot))
            chi[place] = fresh
            total[place] = total[place] + p
            up[place, 8 : 8 + NZ] = (
                up[place, 8 : 8 + NZ]
                - HALF * (press[place, 9 : 9 + NZ] - press[place, 7 : 7 + NZ])
                + (now * slow[1, place] + then * plane(1, 1, slot))
            )
            press[place, 8 : 8 + NZ] = (
                p
                - HALF * (fresh + (up[place, 9 : 9 + NZ] - up[place, 7 : 7 + NZ]))
                + (now * slow[2, place] + then * plane(1, 2, slot))
            )
        return carry

    lax.fori_loop(0, SUBSTEPS, step_body, 0)
    for place, slot in enumerate(slots):
        out[pl.ds(row_out(parities, 0, *slot), NZ, stride=stride_out), :] = total[place]
        out[pl.ds(row_out(parities, 1, *slot), NZ, stride=stride_out), :] = up[place, 8 : 8 + NZ]
        out[pl.ds(row_out(parities, 2, *slot), NZ, stride=stride_out), :] = press[place, 8 : 8 + NZ]


def finish_kernel(got, kept, last, second_back, untwist, slope, across, out, done, sems):
    def modes_of(index, parity):
        rows = [pl.ds(row_out(BOTH, index, parity, part), N2, stride=rows_out(BOTH)) for part in range(2)]
        return jnp.concatenate([got[rows[0], :], got[rows[1], :]], axis=0)

    copies = [pltpu.make_async_copy(done.at[c], out.at[c, 0], sems.at[c]) for c in range(4)]

    def finish(modes, base):
        sides = backward(modes, last, second_back, untwist)
        for index in range(2):
            for rows, cols, value in real_tiles(sides, index):
                done[base + index, rows, cols] = value
            copies[base + index].start()

    finish([jnp.concatenate([modes_of(1, q), modes_of(2, q)], axis=1) for q in BOTH], 2)
    flows = []
    for parity in BOTH:
        total = modes_of(0, parity)
        steep, aside = HALF * slope[parity], HALF * across[0:1]
        flows.append(
            jnp.concatenate(
                [kept[parity, :, :128] - times_i(steep, total), kept[parity, :, 128:] + times_i(aside, total)], axis=1
            )
        )
    finish(flows, 0)
    for copy in copies:
        copy.wait()


VMEM = pl.BlockSpec(memory_space=pltpu.VMEM)
HBM = pl.BlockSpec(memory_space=pltpu.HBM)
ROOM = pltpu.CompilerParams(vmem_limit_bytes=40 * 2**20)


def near(array):
    return pltpu.with_memory_space_constraint(array, pltpu.VMEM)


def local(state, past_slow, mean_wind, damping, vertical_inverse, section):
    axes = ("px", "py")
    rows = rows_in(BOTH)
    message, kept = pl.pallas_call(
        send_kernel,
        out_shape=[pltpu.VMEM((NZ * rows, 128), f32), pltpu.VMEM((2, 2 * N2, 256), f32)],
        in_specs=[HBM] * 10,
        out_specs=[VMEM, VMEM],
        scratch_shapes=[
            pltpu.VMEM((4, NY, NX), f32),
            pltpu.VMEM((4, NY, NX), f32),
            pltpu.VMEM(FIRST.shape, bf16),
            pltpu.VMEM(SECOND.shape, bf16),
            pltpu.VMEM(TWIST.shape, f32),
            pltpu.VMEM(SLOPE.shape, f32),
            pltpu.VMEM(ACROSS.shape, f32),
            pltpu.SMEM((1,), f32),
            pltpu.SMEM((1,), f32),
            pltpu.SMEM((SUBSTEPS,), jnp.int32),
            pltpu.SemaphoreType.DMA((16,)),
        ],
        name="send",
    )(mean_wind, damping, section, state, past_slow, FIRST, SECOND, TWIST, SLOPE, ACROSS)
    moved = lax.all_to_all(message.reshape(NZ, rows, 1, 128), axes, split_axis=0, concat_axis=0, tiled=True)
    arrived = near(moved.reshape(NZ * rows, 128))
    rows = rows_out(BOTH)
    padded = pltpu.VMEM((4, NZ + 16, 128), f32)
    solved = pl.pallas_call(
        lambda *refs: column_kernel(BOTH, *refs),
        out_shape=pltpu.VMEM((NZ * rows, 128), f32),
        in_specs=[HBM, VMEM, VMEM],
        out_specs=VMEM,
        scratch_shapes=[
            pltpu.VMEM((4, NZ, 128), f32),
            pltpu.VMEM((3, 4, NZ, 128), f32),
            padded,
            padded,
            pltpu.VMEM((4, NZ, 128), f32),
            pltpu.SMEM((SUBSTEPS,), jnp.int32),
            pltpu.SemaphoreType.DMA,
        ],
        compiler_params=ROOM,
        name="columns",
    )(section, near(vertical_inverse), arrived)
    back = lax.all_to_all(solved.reshape(NZ, rows // 2, 2, 128), axes, split_axis=0, concat_axis=0, tiled=True)
    returned = near(back.reshape(NZ * rows, 128))
    return pl.pallas_call(
        finish_kernel,
        out_shape=jax.ShapeDtypeStruct((4, 1, NY, NX), f32),
        in_specs=[VMEM] * 7,
        out_specs=HBM,
        scratch_shapes=[pltpu.VMEM((4, NY, NX), f32), pltpu.SemaphoreType.DMA((4,))],
        compiler_params=ROOM,
        name="finish",
    )(returned, near(kept), near(LAST), near(SECOND_BACK), near(UNTWIST), near(SLOPE), near(ACROSS))


def solution(mesh):
    in_specs = (
        P(None, ("px", "py"), None, None),
        P(None, ("px", "py"), None, None),
        P(("px", "py")),
        P(("px", "py")),
        P(),
        P(),
    )
    out_specs = P(None, ("px", "py"), None, None)
    return jax.shard_map(local, mesh=mesh, in_specs=in_specs, out_specs=out_specs, check_vma=False)
```

```python
import math

import jax
import jax.numpy as jnp
import numpy as np
from jax import lax
from jax.experimental import pallas as pl
from jax.experimental.pallas import tpu as pltpu
from jax.sharding import PartitionSpec as P

SUBSTEPS = 8
NX, NY, NZ = 4096, 16, 128
N1, N2 = 32, 128
HN = N1 // 2
TILE = 16
KAP = NY // 2
HALF = 0.275
FAST = 1.0 / SUBSTEPS
NOW = (-1.0, 2.0, 0.5, 1.5)
PAST = (1.0, -0.5, 0.25, -1.0)
BOTH = (0, 1)

f32 = jnp.float32
bf16 = jnp.bfloat16


def halves(table):
    high = np.asarray(jnp.asarray(table, f32).astype(bf16))
    low = np.asarray(jnp.asarray(np.asarray(table, np.float64) - high.astype(np.float64), bf16))
    return np.concatenate([high, low], axis=-1)


def tables():
    y = np.arange(NY)
    kap = np.arange(KAP)
    qa = np.cos(2 * np.pi * kap[:, None] * y[None, :] / NY) * math.sqrt(2.0 / NY)
    qb = np.sin(2 * np.pi * kap[:, None] * y[None, :] / NY) * math.sqrt(2.0 / NY)
    qa[0] = 1.0 / math.sqrt(NY)
    qb[0] = (-1.0) ** y / math.sqrt(NY)
    q = qa + 1j * qb
    n1 = np.arange(HN)
    n2 = np.arange(N2)
    firsts, lasts, twists, untwists = [], [], [], []
    for parity in range(2):
        k1 = 2 * np.arange(HN) + parity
        dft1 = np.exp(-2j * np.pi * (k1[:, None] * n1[None, :] % N1) / N1)
        stage = np.einsum("kn,cy->kcny", dft1, q).reshape(HN, KAP, HN, 2, 8)
        stage = stage.transpose(0, 1, 3, 2, 4).reshape(HN * KAP, 2 * HN * 8)
        first = np.concatenate([stage.real, stage.imag], 0)
        firsts.append(halves(first))
        lasts.append(halves(first.T / NX))
        turn = 2 * np.pi * (k1[:, None] * n2[None, :]) / NX
        twists.append(np.stack([np.cos(turn), np.sin(turn)]))
        wide = np.repeat(turn.T, KAP, axis=1)
        untwists.append(np.stack([np.cos(wide), np.sin(wide)]))
    angle = 2 * np.pi * (n2[:, None] * n2[None, :] % N2) / N2
    cos, sin = np.cos(angle), np.sin(angle)
    second = np.block([[cos, sin], [-sin, cos]])
    k2 = np.arange(N2)
    slopes = []
    for parity in range(2):
        k1 = np.repeat(2 * np.arange(HN) + parity, KAP)
        slopes.append(2 * HALF * np.sin(2 * np.pi * (k1[None, :] + N1 * k2[:, None]) / NX))
    across = np.tile(2 * HALF * np.sin(2 * np.pi * kap / NY), HN)
    return (
        np.stack(firsts),
        np.stack(lasts),
        halves(second),
        halves(second.T),
        np.stack(twists).astype(np.float32),
        np.stack(untwists).astype(np.float32),
        np.stack(slopes).astype(np.float32),
        np.tile(across, (8, 1)).astype(np.float32),
    )


FIRST, LAST, SECOND, SECOND_BACK, TWIST, UNTWIST, SLOPE, ACROSS = tables()


def product(left, right, dims=((1,), (0,))):
    high = right.astype(bf16)
    low = (right - high.astype(f32)).astype(bf16)

    def dot(table, data):
        return lax.dot_general(table, data, (dims, ((), ())), preferred_element_type=f32)

    count = left.shape[0]
    both = dot(jnp.concatenate([left[:, :256], left[:, 256:]], axis=0), high)
    return both[:count] + (both[count:] + dot(left[:, :256], low))


def product_across(left, right):
    return product(left, right, ((1,), (1,)))


def butterfly(plane, parity):
    parts = []
    for b in range(2):
        rows = slice(8 * b, 8 * b + 8)
        for n in range(HN):
            near = plane[rows, N2 * n : N2 * n + N2]
            far = plane[rows, N2 * (n + HN) : N2 * (n + HN) + N2]
            parts.append(near - far if parity else near + far)
    return jnp.concatenate(parts, axis=0)


def forward(planes, parity, first, second, twist):
    columns = jnp.concatenate([butterfly(plane, parity) for plane in planes], axis=1)
    mid = product(first[parity], columns)
    turned = []
    for index in range(2):
        at = slice(N2 * index, N2 * index + N2)
        real, imag = [], []
        for m in range(HN):
            zr, zi = mid[8 * m : 8 * m + 8, at], mid[128 + 8 * m : 128 + 8 * m + 8, at]
            c, s = twist[parity, 0, m : m + 1, :], twist[parity, 1, m : m + 1, :]
            real.append(zr * c + zi * s)
            imag.append(zi * c - zr * s)
        turned.append(jnp.concatenate([jnp.concatenate(real, 0), jnp.concatenate(imag, 0)], axis=1))
    return product_across(second[...], jnp.concatenate(turned, axis=0))


def backward(modes, last, second_back, untwist):
    sides = []
    for parity in range(2):
        mid = product(second_back[...], modes[parity])
        turned = []
        for index in range(mid.shape[1] // 128):
            at = slice(128 * index, 128 * index + 128)
            zr, zi = mid[:N2, at], mid[N2:, at]
            c, s = untwist[parity, 0], untwist[parity, 1]
            turned.append(jnp.concatenate([zr * c - zi * s, zr * s + zi * c], axis=1))
        sides.append(product_across(last[parity], jnp.concatenate(turned, axis=0)))
    return sides


def real_tiles(sides, index):
    at = slice(128 * index, 128 * index + 128)
    for b in range(2):
        for n in range(HN):
            here = slice(8 * (b * HN + n), 8 * (b * HN + n) + 8)
            even, odd = sides[0][here, at], sides[1][here, at]
            rows = slice(8 * b, 8 * b + 8)
            yield rows, slice(N2 * n, N2 * n + N2), even + odd
            yield rows, slice(N2 * (n + HN), N2 * (n + HN) + N2), even - odd


def rows_in(parities):
    return 12 * len(parities) + (1 if 0 in parities else 0)


def rows_out(parities):
    return 6 * len(parities)


def row_in(parities, which, index, parity, part):
    return 12 * parities.index(parity) + 6 * which + 2 * index + part


def row_out(parities, index, parity, part):
    return 6 * parities.index(parity) + 2 * index + part


def weight(section, table, step):
    row = section[step]
    value = jnp.where(row == 3, table[3], 0.0)
    for entry in range(3):
        value = jnp.where(row == entry, table[entry], value)
    return value


def times_i(slope, value):
    return jnp.concatenate([-slope * value[N2:], slope * value[:N2]], axis=0)


def send_kernel(
    wind_in,
    damping_in,
    section_in,
    state,
    past,
    first,
    second,
    twist,
    slope,
    across,
    out,
    kept,
    here,
    then,
    one,
    two,
    tw,
    sl,
    ac,
    wind,
    damping,
    section,
    sems,
):
    copies = {}
    order = [("one", first, one), ("s2", state.at[2, 0], here.at[2]), ("s3", state.at[3, 0], here.at[3])]
    order += [("tw", twist, tw), ("two", second, two)]
    order += [("p2", past.at[2, 0], then.at[2]), ("p3", past.at[3, 0], then.at[3])]
    order += [("s0", state.at[0, 0], here.at[0]), ("s1", state.at[1, 0], here.at[1])]
    order += [("sl", slope, sl), ("ac", across, ac)]
    order += [("p0", past.at[0, 0], then.at[0]), ("p1", past.at[1, 0], then.at[1])]
    order += [("wind", wind_in, wind), ("damping", damping_in, damping), ("section", section_in, section)]
    for number, (name, source, target) in enumerate(order):
        copies[name] = pltpu.make_async_copy(source, target, sems.at[number])
        copies[name].start()
    stride = rows_in(BOTH)

    def put(which, index, parity, modes):
        for part in range(2):
            rows = pl.ds(row_in(BOTH, which, index, parity, part), N2, stride=stride)
            out[rows, :] = modes[N2 * part : N2 * part + N2]

    for name in copies:
        copies[name].wait()
    for parity in range(2):
        modes = forward((here[2], here[3]), parity, one, two, tw)
        put(0, 1, parity, modes[:, :128])
        put(0, 2, parity, modes[:, 128:])
    for parity in range(2):
        modes = forward((then[2], then[3]), parity, one, two, tw)
        put(1, 1, parity, modes[:, :128])
        put(1, 2, parity, modes[:, 128:])
    lane = lax.broadcasted_iota(jnp.int32, (N2, 128), 1)
    out[pl.ds(stride - 1, N2, stride=stride), :] = jnp.where(lane < 64, damping[0], wind[0])
    total_now = weight(section, NOW, 0)
    total_past = weight(section, PAST, 0)
    for step in range(1, SUBSTEPS):
        total_now = total_now + weight(section, NOW, step)
        total_past = total_past + weight(section, PAST, step)
    total_now = total_now * FAST
    total_past = total_past * FAST
    for parity in range(2):
        modes = forward((here[0], here[1]), parity, one, two, tw)
        earlier = forward((then[0], then[1]), parity, one, two, tw)
        steep, aside = sl[parity], ac[0:1]
        put(0, 0, parity, times_i(steep, modes[:, :128]) - times_i(aside, modes[:, 128:]))
        put(1, 0, parity, times_i(steep, earlier[:, :128]) - times_i(aside, earlier[:, 128:]))
        k = lax.broadcasted_iota(jnp.int32, (N2, 128), 0) * N1 + 2 * (lane // KAP) + parity
        fold = jnp.minimum(k, NX - k).astype(f32) * (2.0 / NX)
        fold = fold * fold
        signed = jnp.where(k > NX // 2, k - NX, k)
        signed = jnp.where(k == NX // 2, 0, signed).astype(f32) * (2.0 * math.pi / NX)
        keep = 1.0 - (fold * fold) * (damping[0] * total_now)
        drift = signed * (wind[0] * total_now)
        for index in range(2):
            at = slice(128 * index, 128 * index + 128)
            fr, fi = modes[:N2, at], modes[N2:, at]
            kept[parity, :N2, at] = (keep * fr + drift * fi) + total_past * earlier[:N2, at]
            kept[parity, N2:, at] = (keep * fi - drift * fr) + total_past * earlier[N2:, at]


def lane_tables(index, parity):
    lane = lax.broadcasted_iota(jnp.int32, (8, 128), 1)
    k = index * N1 + 2 * (lane // KAP) + parity
    fold = jnp.minimum(k, NX - k).astype(f32) * (2.0 / NX)
    fold = fold * fold
    signed = jnp.where(k > NX // 2, k - NX, k)
    signed = jnp.where(k == NX // 2, 0, signed).astype(f32) * (2.0 * math.pi / NX)
    sx = jnp.sin(k.astype(f32) * (2.0 * math.pi / NX))
    sy = jnp.sin((lane % KAP).astype(f32) * (2.0 * math.pi / NY))
    coupling = (4.0 * HALF * HALF) * (sx * sx + sy * sy)
    return (fold * fold)[0:1], signed[0:1], coupling[0:1]


def column_kernel(parities, section_in, inverse, got, out, chi, slow, up, press, total, section, sem):
    fetch = pltpu.make_async_copy(section_in, section, sem)
    fetch.start()
    lanes = {parity: lane_tables(lax.axis_index(("px", "py")), parity) for parity in parities}
    zero = jnp.zeros((8, 128), f32)
    stride, stride_out = rows_in(parities), rows_out(parities)
    first_stride = rows_in(BOTH)
    level = got[pl.ds(first_stride - 1, NZ, stride=first_stride), :]
    damping, wind = level[:, 0:1], level[:, 64:65]
    slots = [(parity, part) for parity in parities for part in range(2)]

    def plane(which, index, slot):
        return got[pl.ds(row_in(parities, which, index, *slot), NZ, stride=stride), :]

    for place in range(0, len(slots), 2):
        parity = slots[place][0]
        damp = -damping * lanes[parity][0]
        drift = wind * lanes[parity][1]
        for index in range(3):
            fr, fi = plane(0, index, slots[place]), plane(0, index, slots[place + 1])
            slow[index, place] = damp * fr + drift * fi
            slow[index, place + 1] = damp * fi - drift * fr
            if index == 0:
                chi[place] = fr
                chi[place + 1] = fi
    high = inverse[...].astype(bf16)
    low = (inverse[...] - high.astype(f32)).astype(bf16)
    inv = jnp.concatenate([high, low], axis=1)
    upright = jnp.concatenate(
        [jnp.concatenate([plane(0, index, slot) for slot in slots], axis=1) for index in (1, 2)], axis=0
    )
    solved = product(inv, upright)
    for place in range(len(slots)):
        up[place, 8 : 8 + NZ] = HALF * solved[:NZ, 128 * place : 128 * place + 128]
        press[place, 8 : 8 + NZ] = solved[NZ:, 128 * place : 128 * place + 128]
        total[place] = jnp.zeros((NZ, 128), f32)
        for ref in (up, press):
            ref[place, 0:8] = zero
            ref[place, 8 + NZ : 16 + NZ] = zero

    fetch.wait()

    def step_body(step, carry):
        now = weight(section, NOW, step) * FAST
        then = weight(section, PAST, step) * FAST
        now_up, then_up = now * HALF, then * HALF

        def late(which, index, slot, z):
            return got[pl.ds(row_in(parities, which, index, *slot) + stride * z, TILE, stride=stride), :]

        for place, slot in enumerate(slots):
            for z in range(0, NZ, TILE):
                here = slice(z, z + TILE)
                p = press[place, 8 + z : 8 + z + TILE]
                total[place, here] = total[place, here] + p
                chi[place, here] = (
                    chi[place, here]
                    + lanes[slot[0]][2] * p
                    + (now * slow[0, place, here] + then * late(1, 0, slot, z))
                )
                up[place, 8 + z : 8 + z + TILE] = (
                    up[place, 8 + z : 8 + z + TILE]
                    - (HALF * HALF) * (press[place, 9 + z : 9 + z + TILE] - press[place, 7 + z : 7 + z + TILE])
                    + (now_up * slow[1, place, here] + then_up * late(1, 1, slot, z))
                )
            for z in range(0, NZ, TILE):
                here = slice(z, z + TILE)
                press[place, 8 + z : 8 + z + TILE] = (
                    press[place, 8 + z : 8 + z + TILE]
                    - (chi[place, here] + (up[place, 9 + z : 9 + z + TILE] - up[place, 7 + z : 7 + z + TILE]))
                    + (now * slow[2, place, here] + then * late(1, 2, slot, z))
                )
        return carry

    lax.fori_loop(0, SUBSTEPS, step_body, 0)
    for place, slot in enumerate(slots):
        out[pl.ds(row_out(parities, 0, *slot), NZ, stride=stride_out), :] = total[place]
        out[pl.ds(row_out(parities, 1, *slot), NZ, stride=stride_out), :] = up[place, 8 : 8 + NZ] * (1.0 / HALF)
        out[pl.ds(row_out(parities, 2, *slot), NZ, stride=stride_out), :] = press[place, 8 : 8 + NZ]


def finish_kernel(got, kept, last, second_back, untwist, slope, across, out, done, sems):
    def modes_of(index, parity):
        rows = [pl.ds(row_out(BOTH, index, parity, part), N2, stride=rows_out(BOTH)) for part in range(2)]
        return jnp.concatenate([got[rows[0], :], got[rows[1], :]], axis=0)

    copies = [pltpu.make_async_copy(done.at[c], out.at[c, 0], sems.at[c]) for c in range(4)]

    def finish(modes, base):
        sides = backward(modes, last, second_back, untwist)
        for index in range(2):
            for rows, cols, value in real_tiles(sides, index):
                done[base + index, rows, cols] = value
            copies[base + index].start()

    finish([jnp.concatenate([modes_of(1, q), modes_of(2, q)], axis=1) for q in BOTH], 2)
    flows = []
    for parity in BOTH:
        total = modes_of(0, parity)
        steep, aside = slope[parity], across[0:1]
        flows.append(
            jnp.concatenate(
                [kept[parity, :, :128] - times_i(steep, total), kept[parity, :, 128:] + times_i(aside, total)], axis=1
            )
        )
    finish(flows, 0)
    for copy in copies:
        copy.wait()


VMEM = pl.BlockSpec(memory_space=pltpu.VMEM)
HBM = pl.BlockSpec(memory_space=pltpu.HBM)
ROOM = pltpu.CompilerParams(vmem_limit_bytes=40 * 2**20)


def near(array):
    return pltpu.with_memory_space_constraint(array, pltpu.VMEM)


def local(state, past_slow, mean_wind, damping, vertical_inverse, section):
    axes = ("px", "py")
    rows = rows_in(BOTH)
    message, kept = pl.pallas_call(
        send_kernel,
        out_shape=[pltpu.VMEM((NZ * rows, 128), f32), pltpu.VMEM((2, 2 * N2, 256), f32)],
        in_specs=[HBM] * 10,
        out_specs=[VMEM, VMEM],
        scratch_shapes=[
            pltpu.VMEM((4, NY, NX), f32),
            pltpu.VMEM((4, NY, NX), f32),
            pltpu.VMEM(FIRST.shape, bf16),
            pltpu.VMEM(SECOND.shape, bf16),
            pltpu.VMEM(TWIST.shape, f32),
            pltpu.VMEM(SLOPE.shape, f32),
            pltpu.VMEM(ACROSS.shape, f32),
            pltpu.SMEM((1,), f32),
            pltpu.SMEM((1,), f32),
            pltpu.SMEM((SUBSTEPS,), jnp.int32),
            pltpu.SemaphoreType.DMA((16,)),
        ],
        name="send",
    )(mean_wind, damping, section, state, past_slow, FIRST, SECOND, TWIST, SLOPE, ACROSS)
    moved = lax.all_to_all(message.reshape(NZ, rows, 1, 128), axes, split_axis=0, concat_axis=0, tiled=True)
    arrived = near(moved.reshape(NZ * rows, 128))
    rows = rows_out(BOTH)
    padded = pltpu.VMEM((4, NZ + 16, 128), f32)
    solved = pl.pallas_call(
        lambda *refs: column_kernel(BOTH, *refs),
        out_shape=pltpu.VMEM((NZ * rows, 128), f32),
        in_specs=[HBM, VMEM, VMEM],
        out_specs=VMEM,
        scratch_shapes=[
            pltpu.VMEM((4, NZ, 128), f32),
            pltpu.VMEM((3, 4, NZ, 128), f32),
            padded,
            padded,
            pltpu.VMEM((4, NZ, 128), f32),
            pltpu.SMEM((SUBSTEPS,), jnp.int32),
            pltpu.SemaphoreType.DMA,
        ],
        compiler_params=ROOM,
        name="columns",
    )(section, near(vertical_inverse), arrived)
    back = lax.all_to_all(solved.reshape(NZ, rows // 2, 2, 128), axes, split_axis=0, concat_axis=0, tiled=True)
    returned = near(back.reshape(NZ * rows, 128))
    return pl.pallas_call(
        finish_kernel,
        out_shape=jax.ShapeDtypeStruct((4, 1, NY, NX), f32),
        in_specs=[VMEM] * 7,
        out_specs=HBM,
        scratch_shapes=[pltpu.VMEM((4, NY, NX), f32), pltpu.SemaphoreType.DMA((4,))],
        compiler_params=ROOM,
        name="finish",
    )(returned, near(kept), near(LAST), near(SECOND_BACK), near(UNTWIST), near(SLOPE), near(ACROSS))


def solution(mesh):
    in_specs = (
        P(None, ("px", "py"), None, None),
        P(None, ("px", "py"), None, None),
        P(("px", "py")),
        P(("px", "py")),
        P(),
        P(),
    )
    out_specs = P(None, ("px", "py"), None, None)
    return jax.shard_map(local, mesh=mesh, in_specs=in_specs, out_specs=out_specs, check_vma=False)
```

```python
import math

import jax
import jax.numpy as jnp
import numpy as np
from jax import lax
from jax.experimental import pallas as pl
from jax.experimental.pallas import tpu as pltpu
from jax.sharding import PartitionSpec as P

SUBSTEPS = 8
NX, NY, NZ = 4096, 16, 128
N1, N2 = 32, 128
HN = N1 // 2
TILE = 16
KAP = NY // 2
HALF = 0.275
FAST = 1.0 / SUBSTEPS
NOW = (-1.0, 2.0, 0.5, 1.5)
PAST = (1.0, -0.5, 0.25, -1.0)
BOTH = (0, 1)

f32 = jnp.float32
bf16 = jnp.bfloat16


def halves(table):
    high = np.asarray(jnp.asarray(table, f32).astype(bf16))
    low = np.asarray(jnp.asarray(np.asarray(table, np.float64) - high.astype(np.float64), bf16))
    return np.concatenate([high, low], axis=-1)


def tables():
    y = np.arange(NY)
    kap = np.arange(KAP)
    qa = np.cos(2 * np.pi * kap[:, None] * y[None, :] / NY) * math.sqrt(2.0 / NY)
    qb = np.sin(2 * np.pi * kap[:, None] * y[None, :] / NY) * math.sqrt(2.0 / NY)
    qa[0] = 1.0 / math.sqrt(NY)
    qb[0] = (-1.0) ** y / math.sqrt(NY)
    q = qa + 1j * qb
    n1 = np.arange(HN)
    n2 = np.arange(N2)
    firsts, lasts, twists, untwists = [], [], [], []
    for parity in range(2):
        k1 = 2 * np.arange(HN) + parity
        dft1 = np.exp(-2j * np.pi * (k1[:, None] * n1[None, :] % N1) / N1)
        stage = np.einsum("kn,cy->kcny", dft1, q).reshape(HN, KAP, HN, 2, 8)
        stage = stage.transpose(0, 1, 3, 2, 4).reshape(HN * KAP, 2 * HN * 8)
        first = np.concatenate([stage.real, stage.imag], 0)
        firsts.append(halves(first))
        lasts.append(halves(first.T / NX))
        turn = 2 * np.pi * (k1[:, None] * n2[None, :]) / NX
        twists.append(np.stack([np.cos(turn), np.sin(turn)]))
        wide = np.repeat(turn.T, KAP, axis=1)
        untwists.append(np.stack([np.cos(wide), np.sin(wide)]))
    angle = 2 * np.pi * (n2[:, None] * n2[None, :] % N2) / N2
    cos, sin = np.cos(angle), np.sin(angle)
    second = np.block([[cos, sin], [-sin, cos]])
    k2 = np.arange(N2)
    slopes = []
    for parity in range(2):
        k1 = np.repeat(2 * np.arange(HN) + parity, KAP)
        slopes.append(2 * HALF * np.sin(2 * np.pi * (k1[None, :] + N1 * k2[:, None]) / NX))
    across = np.tile(2 * HALF * np.sin(2 * np.pi * kap / NY), HN)
    return (
        np.stack(firsts),
        np.stack(lasts),
        halves(second),
        halves(second.T),
        np.stack(twists).astype(np.float32),
        np.stack(untwists).astype(np.float32),
        np.stack(slopes).astype(np.float32),
        np.tile(across, (8, 1)).astype(np.float32),
    )


FIRST, LAST, SECOND, SECOND_BACK, TWIST, UNTWIST, SLOPE, ACROSS = tables()


def product(left, right, dims=((1,), (0,))):
    high = right.astype(bf16)
    low = (right - high.astype(f32)).astype(bf16)

    def dot(table, data):
        return lax.dot_general(table, data, (dims, ((), ())), preferred_element_type=f32)

    count = left.shape[0]
    both = dot(jnp.concatenate([left[:, :256], left[:, 256:]], axis=0), high)
    return both[:count] + (both[count:] + dot(left[:, :256], low))


def deep(left, right, axis, dims):
    high = right.astype(bf16)
    low = (right - high.astype(f32)).astype(bf16)
    table = jnp.concatenate([left[...], left[:, :256]], axis=1)
    data = jnp.concatenate([high, high, low], axis=axis)
    return lax.dot_general(table, data, (dims, ((), ())), preferred_element_type=f32)


def product_across(left, right):
    return deep(left, right, 1, ((1,), (1,)))


def butterfly(plane, parity):
    parts = []
    for b in range(2):
        rows = slice(8 * b, 8 * b + 8)
        for n in range(HN):
            near = plane[rows, N2 * n : N2 * n + N2]
            far = plane[rows, N2 * (n + HN) : N2 * (n + HN) + N2]
            parts.append(near - far if parity else near + far)
    return jnp.concatenate(parts, axis=0)


def forward(planes, parity, first, second, twist):
    columns = jnp.concatenate([butterfly(plane, parity) for plane in planes], axis=1)
    mid = product(first[parity], columns)
    turned = []
    for index in range(2):
        at = slice(N2 * index, N2 * index + N2)
        real, imag = [], []
        for m in range(HN):
            zr, zi = mid[8 * m : 8 * m + 8, at], mid[128 + 8 * m : 128 + 8 * m + 8, at]
            c, s = twist[parity, 0, m : m + 1, :], twist[parity, 1, m : m + 1, :]
            real.append(zr * c + zi * s)
            imag.append(zi * c - zr * s)
        turned.append(jnp.concatenate([jnp.concatenate(real, 0), jnp.concatenate(imag, 0)], axis=1))
    return product_across(second[...], jnp.concatenate(turned, axis=0))


def backward(modes, last, second_back, untwist):
    sides = []
    for parity in range(2):
        mid = product(second_back[...], modes[parity])
        turned = []
        for index in range(mid.shape[1] // 128):
            at = slice(128 * index, 128 * index + 128)
            zr, zi = mid[:N2, at], mid[N2:, at]
            c, s = untwist[parity, 0], untwist[parity, 1]
            turned.append(jnp.concatenate([zr * c - zi * s, zr * s + zi * c], axis=1))
        sides.append(product_across(last[parity], jnp.concatenate(turned, axis=0)))
    return sides


def real_tiles(sides, index):
    at = slice(128 * index, 128 * index + 128)
    for b in range(2):
        for n in range(HN):
            here = slice(8 * (b * HN + n), 8 * (b * HN + n) + 8)
            even, odd = sides[0][here, at], sides[1][here, at]
            rows = slice(8 * b, 8 * b + 8)
            yield rows, slice(N2 * n, N2 * n + N2), even + odd
            yield rows, slice(N2 * (n + HN), N2 * (n + HN) + N2), even - odd


def rows_in(parities):
    return 12 * len(parities) + (1 if 0 in parities else 0)


def rows_out(parities):
    return 6 * len(parities)


def row_in(parities, which, index, parity, part):
    return 12 * parities.index(parity) + 6 * which + 2 * index + part


def row_out(parities, index, parity, part):
    return 6 * parities.index(parity) + 2 * index + part


def weight(section, table, step):
    row = section[step]
    value = jnp.where(row == 3, table[3], 0.0)
    for entry in range(3):
        value = jnp.where(row == entry, table[entry], value)
    return value


def times_i(slope, value):
    return jnp.concatenate([-slope * value[N2:], slope * value[:N2]], axis=0)


def send_kernel(
    wind_in,
    damping_in,
    section_in,
    state,
    past,
    first,
    second,
    twist,
    slope,
    across,
    out,
    kept,
    here,
    then,
    one,
    two,
    tw,
    sl,
    ac,
    wind,
    damping,
    section,
    sems,
):
    copies = {}
    order = [("state", state.at[:, 0], here), ("past", past.at[:, 0], then), ("one", first, one)]
    order += [("two", second, two), ("slope", slope, sl), ("tw", twist, tw), ("ac", across, ac)]
    order += [("wind", wind_in, wind), ("damping", damping_in, damping), ("section", section_in, section)]
    for number, (name, source, target) in enumerate(order):
        copies[name] = pltpu.make_async_copy(source, target, sems.at[number])
        copies[name].start()
    stride = rows_in(BOTH)

    def put(which, index, parity, modes):
        for part in range(2):
            rows = pl.ds(row_in(BOTH, which, index, parity, part), N2, stride=stride)
            out[rows, :] = modes[N2 * part : N2 * part + N2]

    for name in copies:
        copies[name].wait()
    for parity in range(2):
        modes = forward((here[2], here[3]), parity, one, two, tw)
        put(0, 1, parity, modes[:, :128])
        put(0, 2, parity, modes[:, 128:])
    for parity in range(2):
        modes = forward((then[2], then[3]), parity, one, two, tw)
        put(1, 1, parity, modes[:, :128])
        put(1, 2, parity, modes[:, 128:])
    lane = lax.broadcasted_iota(jnp.int32, (N2, 128), 1)
    out[pl.ds(stride - 1, N2, stride=stride), :] = jnp.where(lane < 64, damping[0], wind[0])
    total_now = weight(section, NOW, 0)
    total_past = weight(section, PAST, 0)
    for step in range(1, SUBSTEPS):
        total_now = total_now + weight(section, NOW, step)
        total_past = total_past + weight(section, PAST, step)
    total_now = total_now * FAST
    total_past = total_past * FAST
    for parity in range(2):
        modes = forward((here[0], here[1]), parity, one, two, tw)
        earlier = forward((then[0], then[1]), parity, one, two, tw)
        steep, aside = sl[parity], ac[0:1]
        put(0, 0, parity, times_i(steep, modes[:, :128]) - times_i(aside, modes[:, 128:]))
        put(1, 0, parity, times_i(steep, earlier[:, :128]) - times_i(aside, earlier[:, 128:]))
        k = lax.broadcasted_iota(jnp.int32, (N2, 128), 0) * N1 + 2 * (lane // KAP) + parity
        fold = jnp.minimum(k, NX - k).astype(f32) * (2.0 / NX)
        fold = fold * fold
        signed = jnp.where(k > NX // 2, k - NX, k)
        signed = jnp.where(k == NX // 2, 0, signed).astype(f32) * (2.0 * math.pi / NX)
        keep = 1.0 - (fold * fold) * (damping[0] * total_now)
        drift = signed * (wind[0] * total_now)
        for index in range(2):
            at = slice(128 * index, 128 * index + 128)
            fr, fi = modes[:N2, at], modes[N2:, at]
            kept[parity, :N2, at] = (keep * fr + drift * fi) + total_past * earlier[:N2, at]
            kept[parity, N2:, at] = (keep * fi - drift * fr) + total_past * earlier[N2:, at]


def lane_tables(index, parity):
    lane = lax.broadcasted_iota(jnp.int32, (8, 128), 1)
    k = index * N1 + 2 * (lane // KAP) + parity
    fold = jnp.minimum(k, NX - k).astype(f32) * (2.0 / NX)
    fold = fold * fold
    signed = jnp.where(k > NX // 2, k - NX, k)
    signed = jnp.where(k == NX // 2, 0, signed).astype(f32) * (2.0 * math.pi / NX)
    sx = jnp.sin(k.astype(f32) * (2.0 * math.pi / NX))
    sy = jnp.sin((lane % KAP).astype(f32) * (2.0 * math.pi / NY))
    coupling = (4.0 * HALF * HALF) * (sx * sx + sy * sy)
    return (fold * fold)[0:1], signed[0:1], coupling[0:1]


def column_kernel(parities, section_in, inverse, got, out, chi, slow, up, press, total, section, sem):
    fetch = pltpu.make_async_copy(section_in, section, sem)
    fetch.start()
    lanes = {parity: lane_tables(lax.axis_index(("px", "py")), parity) for parity in parities}
    zero = jnp.zeros((8, 128), f32)
    stride, stride_out = rows_in(parities), rows_out(parities)
    first_stride = rows_in(BOTH)
    level = got[pl.ds(first_stride - 1, NZ, stride=first_stride), :]
    damping, wind = level[:, 0:1], level[:, 64:65]
    slots = [(parity, part) for parity in parities for part in range(2)]

    def plane(which, index, slot):
        return got[pl.ds(row_in(parities, which, index, *slot), NZ, stride=stride), :]

    for place in range(0, len(slots), 2):
        parity = slots[place][0]
        damp = -damping * lanes[parity][0]
        drift = wind * lanes[parity][1]
        for index in range(3):
            fr, fi = plane(0, index, slots[place]), plane(0, index, slots[place + 1])
            slow[index, place] = damp * fr + drift * fi
            slow[index, place + 1] = damp * fi - drift * fr
            if index == 0:
                chi[place] = fr
                chi[place + 1] = fi
    high = inverse[...].astype(bf16)
    low = (inverse[...] - high.astype(f32)).astype(bf16)
    inv = jnp.concatenate([high, low], axis=1)
    upright = jnp.concatenate(
        [jnp.concatenate([plane(0, index, slot) for slot in slots], axis=1) for index in (1, 2)], axis=0
    )
    solved = product(inv, upright)
    for place in range(len(slots)):
        up[place, 8 : 8 + NZ] = HALF * solved[:NZ, 128 * place : 128 * place + 128]
        press[place, 8 : 8 + NZ] = solved[NZ:, 128 * place : 128 * place + 128]
        total[place] = jnp.zeros((NZ, 128), f32)
        for ref in (up, press):
            ref[place, 0:8] = zero
            ref[place, 8 + NZ : 16 + NZ] = zero

    fetch.wait()

    def step_body(step, carry):
        now = weight(section, NOW, step) * FAST
        then = weight(section, PAST, step) * FAST
        now_up, then_up = now * HALF, then * HALF

        def late(which, index, slot, z):
            return got[pl.ds(row_in(parities, which, index, *slot) + stride * z, TILE, stride=stride), :]

        for place, slot in enumerate(slots):
            for z in range(0, NZ, TILE):
                here = slice(z, z + TILE)
                p = press[place, 8 + z : 8 + z + TILE]
                total[place, here] = total[place, here] + p
                chi[place, here] = (
                    chi[place, here]
                    + lanes[slot[0]][2] * p
                    + (now * slow[0, place, here] + then * late(1, 0, slot, z))
                )
                up[place, 8 + z : 8 + z + TILE] = (
                    up[place, 8 + z : 8 + z + TILE]
                    - (HALF * HALF) * (press[place, 9 + z : 9 + z + TILE] - press[place, 7 + z : 7 + z + TILE])
                    + (now_up * slow[1, place, here] + then_up * late(1, 1, slot, z))
                )
            for z in range(0, NZ, TILE):
                here = slice(z, z + TILE)
                press[place, 8 + z : 8 + z + TILE] = (
                    press[place, 8 + z : 8 + z + TILE]
                    - (chi[place, here] + (up[place, 9 + z : 9 + z + TILE] - up[place, 7 + z : 7 + z + TILE]))
                    + (now * slow[2, place, here] + then * late(1, 2, slot, z))
                )
        return carry

    lax.fori_loop(0, SUBSTEPS, step_body, 0)
    for place, slot in enumerate(slots):
        out[pl.ds(row_out(parities, 0, *slot), NZ, stride=stride_out), :] = total[place]
        out[pl.ds(row_out(parities, 1, *slot), NZ, stride=stride_out), :] = up[place, 8 : 8 + NZ] * (1.0 / HALF)
        out[pl.ds(row_out(parities, 2, *slot), NZ, stride=stride_out), :] = press[place, 8 : 8 + NZ]


def finish_kernel(got, kept, last, second_back, untwist, slope, across, out, done, sems):
    def modes_of(index, parity):
        rows = [pl.ds(row_out(BOTH, index, parity, part), N2, stride=rows_out(BOTH)) for part in range(2)]
        return jnp.concatenate([got[rows[0], :], got[rows[1], :]], axis=0)

    copies = [pltpu.make_async_copy(done.at[c], out.at[c, 0], sems.at[c]) for c in range(4)]

    def finish(modes, base):
        sides = backward(modes, last, second_back, untwist)
        for index in range(2):
            for rows, cols, value in real_tiles(sides, index):
                done[base + index, rows, cols] = value
            copies[base + index].start()

    finish([jnp.concatenate([modes_of(1, q), modes_of(2, q)], axis=1) for q in BOTH], 2)
    flows = []
    for parity in BOTH:
        total = modes_of(0, parity)
        steep, aside = slope[parity], across[0:1]
        flows.append(
            jnp.concatenate(
                [kept[parity, :, :128] - times_i(steep, total), kept[parity, :, 128:] + times_i(aside, total)], axis=1
            )
        )
    finish(flows, 0)
    for copy in copies:
        copy.wait()


VMEM = pl.BlockSpec(memory_space=pltpu.VMEM)
HBM = pl.BlockSpec(memory_space=pltpu.HBM)
ROOM = pltpu.CompilerParams(vmem_limit_bytes=40 * 2**20)


def near(array):
    return pltpu.with_memory_space_constraint(array, pltpu.VMEM)


def local(state, past_slow, mean_wind, damping, vertical_inverse, section):
    axes = ("px", "py")
    rows = rows_in(BOTH)
    message, kept = pl.pallas_call(
        send_kernel,
        out_shape=[pltpu.VMEM((NZ * rows, 128), f32), pltpu.VMEM((2, 2 * N2, 256), f32)],
        in_specs=[HBM] * 10,
        out_specs=[VMEM, VMEM],
        scratch_shapes=[
            pltpu.VMEM((4, NY, NX), f32),
            pltpu.VMEM((4, NY, NX), f32),
            pltpu.VMEM(FIRST.shape, bf16),
            pltpu.VMEM(SECOND.shape, bf16),
            pltpu.VMEM(TWIST.shape, f32),
            pltpu.VMEM(SLOPE.shape, f32),
            pltpu.VMEM(ACROSS.shape, f32),
            pltpu.SMEM((1,), f32),
            pltpu.SMEM((1,), f32),
            pltpu.SMEM((SUBSTEPS,), jnp.int32),
            pltpu.SemaphoreType.DMA((10,)),
        ],
        name="send",
    )(mean_wind, damping, section, state, past_slow, FIRST, SECOND, TWIST, SLOPE, ACROSS)
    moved = lax.all_to_all(message.reshape(NZ, rows, 1, 128), axes, split_axis=0, concat_axis=0, tiled=True)
    arrived = near(moved.reshape(NZ * rows, 128))
    rows = rows_out(BOTH)
    padded = pltpu.VMEM((4, NZ + 16, 128), f32)
    solved = pl.pallas_call(
        lambda *refs: column_kernel(BOTH, *refs),
        out_shape=pltpu.VMEM((NZ * rows, 128), f32),
        in_specs=[HBM, VMEM, VMEM],
        out_specs=VMEM,
        scratch_shapes=[
            pltpu.VMEM((4, NZ, 128), f32),
            pltpu.VMEM((3, 4, NZ, 128), f32),
            padded,
            padded,
            pltpu.VMEM((4, NZ, 128), f32),
            pltpu.SMEM((SUBSTEPS,), jnp.int32),
            pltpu.SemaphoreType.DMA,
        ],
        compiler_params=ROOM,
        name="columns",
    )(section, near(vertical_inverse), arrived)
    back = lax.all_to_all(solved.reshape(NZ, rows // 2, 2, 128), axes, split_axis=0, concat_axis=0, tiled=True)
    returned = near(back.reshape(NZ * rows, 128))
    return pl.pallas_call(
        finish_kernel,
        out_shape=jax.ShapeDtypeStruct((4, 1, NY, NX), f32),
        in_specs=[VMEM] * 7,
        out_specs=HBM,
        scratch_shapes=[pltpu.VMEM((4, NY, NX), f32), pltpu.SemaphoreType.DMA((4,))],
        compiler_params=ROOM,
        name="finish",
    )(returned, near(kept), near(LAST), near(SECOND_BACK), near(UNTWIST), near(SLOPE), near(ACROSS))


def solution(mesh):
    in_specs = (
        P(None, ("px", "py"), None, None),
        P(None, ("px", "py"), None, None),
        P(("px", "py")),
        P(("px", "py")),
        P(),
        P(),
    )
    out_specs = P(None, ("px", "py"), None, None)
    return jax.shard_map(local, mesh=mesh, in_specs=in_specs, out_specs=out_specs, check_vma=False)
```
